8 devices in a mesh: dp: 1 (over z), tp: 8 (over x, y, core).
Axes of the slice: x: 2, y: 2, z: 1, core: 2. Of those that a mesh axis runs over, the one named last changes fastest.
Arguments:
- x: bfloat16 [2048, 12288], P('dp')
- gain: bfloat16 [12288], replicated
- wq: bfloat16 [12288, 12288], P(None, 'tp')
- wk: bfloat16 [12288, 1024], P(None, 'tp')
- wv: bfloat16 [12288, 1024], P(None, 'tp')
- wo: bfloat16 [12288, 12288], P('tp')
Outputs:
- output: bfloat16 [2048, 12288], P('dp')
All inputs are finite; a program needn't handle non-finite values.
Results may differ from the reference program's by a relative error of at most 0.012.
Values are sent between devices in bfloat16 or wider.
A program may use at most 2 GiB of HBM per device.

```python
import jax
import jax.numpy as jnp
from jax import lax

ROWS = 2048
D = 12288
HEADS = 96
KV_HEADS = 8
HEAD = 128
THETA = 10000


def setup_inputs(seed: int = 0, part: int = 0) -> dict:
    kx, kn, kq, kk, kv, ko = jax.random.split(jax.random.key(seed), 6)

    def weights(key, rows, columns):
        return jax.random.normal(key, (rows, columns), jnp.float32) * rows**-0.5

    drawn = {
        "x": jax.random.normal(jax.random.fold_in(kx, part), (ROWS, D), jnp.float32),
        "gain": 1 + 0.1 * jax.random.normal(kn, (D,), jnp.float32),
        "wq": 2 * weights(kq, D, HEADS * HEAD),
        "wk": 2 * weights(kk, D, KV_HEADS * HEAD),
        "wv": 4 * weights(kv, D, KV_HEADS * HEAD),
        "wo": weights(ko, HEADS * HEAD, D),
    }
    return {k: v.astype(jnp.bfloat16) for k, v in drawn.items()}


def normed(x, gain):
    wide = x.astype(jnp.float32)
    scale = lax.rsqrt(jnp.mean(wide * wide, -1, keepdims=True) + 1e-6)
    return (wide * scale * gain.astype(jnp.float32)).astype(jnp.bfloat16)


def turned(t, place, theta):
    half = t.shape[-1] // 2
    angle = place.astype(jnp.float32)[:, None] * theta ** (-jnp.arange(half, dtype=jnp.float32) / half)
    cos, sin = jnp.cos(angle)[:, None], jnp.sin(angle)[:, None]
    a, b = t[..., :half].astype(jnp.float32), t[..., half:].astype(jnp.float32)
    return jnp.concatenate([a * cos - b * sin, b * cos + a * sin], -1).astype(jnp.bfloat16)


def matmul(a, w):
    return jnp.dot(a, w, preferred_element_type=jnp.float32).astype(jnp.bfloat16)


def einsum(form, a, b):
    return jnp.einsum(form, a.astype(jnp.float32), b.astype(jnp.float32))


def attention(q, k, v):
    scores = einsum("tgsd,ugd->gstu", q, k) * q.shape[-1] ** -0.5
    token = jnp.arange(q.shape[0])
    scores = jnp.where(token[:, None] >= token, scores, -jnp.inf)
    weights = jax.nn.softmax(scores, -1).astype(jnp.bfloat16)
    return einsum("gstu,ugd->tgsd", weights, v).astype(jnp.bfloat16)


def reference(x, gain, wq, wk, wv, wo):
    a, place = normed(x, gain), jnp.arange(ROWS)
    q = turned(matmul(a, wq).reshape(ROWS, HEADS, HEAD), place, THETA).reshape(ROWS, KV_HEADS, -1, HEAD)
    k = turned(matmul(a, wk).reshape(ROWS, KV_HEADS, HEAD), place, THETA)
    v = matmul(a, wv).reshape(ROWS, KV_HEADS, HEAD)
    seen = attention(q, k, v).reshape(ROWS, HEADS * HEAD)
    return (x.astype(jnp.float32) + jnp.dot(seen, wo, preferred_element_type=jnp.float32)).astype(jnp.bfloat16)
```

```python
import functools

import jax
import jax.numpy as jnp
import numpy as np
from jax import lax
from jax.experimental import pallas as pl
from jax.experimental.pallas import tpu as pltpu
from jax.sharding import PartitionSpec as P

HEAD = 128
THETA = 10000
NEG = -1e30
HIDDEN = 2 * NEG
LOG2E = 1.4426950408889634
E = HEAD**-0.5 * LOG2E
ROWS, D = 2048, 12288
R = 256
S = 12
BN = D // S
RB = 64
BK = 512
C = ROWS // R
UNITS = C * S
N = R // 16
SLOTS = 4
J1, J2, J3, F4, F5, F6 = 1, 3, 5, 7, 9, 11
STEPS = S + UNITS + F6


def _dot(a, b, ca, cb):
    return lax.dot_general(a, b, (((ca,), (cb,)), ((), ())), preferred_element_type=jnp.float32)


def _table():
    half = HEAD // 2
    freq = (np.float32(THETA) ** (-np.arange(half, dtype=np.float32) / np.float32(half))).astype(np.float32)
    angle = np.arange(ROWS, dtype=np.float32)[:, None] * freq
    return np.concatenate([np.cos(angle), np.sin(angle)], axis=1).astype(np.float32)


def _turn(t, table):
    half = HEAD // 2
    a, b, cos, sin = t[:, :half], t[:, half:], table[:, :half], table[:, half:]
    return jnp.concatenate([a * cos - b * sin, b * cos + a * sin], axis=1).astype(jnp.bfloat16)


def _kernel(x_ref, gain_ref, wq_ref, wo_ref, table_ref, x_hbm, wk_hbm, wv_hbm, y_hbm,
            normed_s, wkv_s, k_s, vt_s, seen_s, q_s, top_s, mix_s,
            send0, keep0, recv0, send1, keep1, recv1, send2, keep2, recv2, res_s, fin_s,
            w_sem, s0, r0, s1, r1, s2, r2, s3, r3, s4, r4, s5, r5, res_sem, fin_sem):
    g = pl.program_id(0)
    t, n = lax.div(g, S), lax.rem(g, S)
    me = lax.axis_index("tp")
    core, yb, xb = lax.rem(me, 2), lax.rem(lax.div(me, 2), 2), lax.div(me, 4)
    to_core, to_y, to_x = me + 1 - 2 * core, me + 2 - 4 * yb, me + 4 - 8 * xb
    first, second = (xb, yb), (yb, xb)
    to_first, to_second = (to_x, to_y), (to_y, to_x)

    def remote(src, dst, send_sem, recv_sem, to):
        return pltpu.make_async_remote_copy(src_ref=src, dst_ref=dst, send_sem=send_sem, recv_sem=recv_sem, device_id={"tp": to},
                                            device_id_type=pl.DeviceIdType.MESH)

    def rows_of(u, piece, count):
        row = pl.multiple_of(lax.div(u, S) * R + piece * N, N)
        return pl.ds(row, count * N), pl.ds(pl.multiple_of(lax.rem(u, S) * BN, BN), BN)

    def own(h):
        return core * 8 + h * 4 + first[h] * 2 + second[h]

    def weights():
        return [pltpu.make_async_copy(w, wkv_s.at[:, pl.ds(i * HEAD, HEAD)], w_sem.at[i]) for i, w in enumerate((wk_hbm, wv_hbm))]

    def sum0(u):
        a, b = lax.rem(u, 2), lax.rem(u, SLOTS)
        return remote(send0.at[a], recv0.at[b], s0.at[b], r0.at[b], to_core)

    def sum1(u, h):
        b = lax.rem(u, SLOTS)
        return remote(send1.at[b, h], recv1.at[b, h], s1.at[b, h], r1.at[b, h], to_first[h])

    def sum2(u, h):
        b = lax.rem(u, SLOTS)
        return remote(send2.at[b, h], recv2.at[b, h], s2.at[b, h], r2.at[b, h], to_second[h])

    def residual(u, h):
        b = lax.rem(u, SLOTS)
        return pltpu.make_async_copy(x_hbm.at[rows_of(u, own(h), 1)], res_s.at[b, h], res_sem.at[b, h])

    def stay(u, h):
        b = lax.rem(u, SLOTS)
        return pltpu.make_async_copy(fin_s.at[b, h], y_hbm.at[rows_of(u, own(h), 1)], fin_sem.at[b, h])

    def back3(u, h):
        b = lax.rem(u, SLOTS)
        return remote(fin_s.at[b, h], y_hbm.at[rows_of(u, own(h), 1)], s3.at[b, h], r3.at[b, h], to_second[h])

    def back4(u, h):
        b = lax.rem(u, SLOTS)
        at = rows_of(u, core * 8 + h * 4 + first[h] * 2, 2)
        return remote(y_hbm.at[at], y_hbm.at[at], s4.at[b, h], r4.at[b, h], to_first[h])

    def back5(u):
        b = lax.rem(u, SLOTS)
        at = rows_of(u, core * 8, 8)
        return remote(y_hbm.at[at], y_hbm.at[at], s5.at[b], r5.at[b], to_core)

    @pl.when(g == 0)
    def _():
        barrier = pltpu.get_barrier_semaphore()
        for to in (to_core, to_y, to_x):
            pl.semaphore_signal(barrier, inc=1, device_id={"tp": to}, device_id_type=pl.DeviceIdType.MESH)
        pl.semaphore_wait(barrier, 3)
        for w in weights():
            w.start()
        k_s[...] = jnp.zeros_like(k_s)
        vt_s[...] = jnp.zeros_like(vt_s)
        vt_s[HEAD:, :] = jnp.ones((16, ROWS), vt_s.dtype)

    def at_step(lag):
        u = g - S - lag
        return u, (u >= 0) & (u < UNITS)

    u6, on6 = at_step(F6)

    @pl.when(on6)
    def _():
        back5(u6).wait()

    u5, on5 = at_step(F5)

    @pl.when(on5)
    def _():
        for h in range(2):
            back4(u5, h).wait()
        back5(u5).start()

    u4, on4 = at_step(F4)

    @pl.when(on4)
    def _():
        for h in range(2):
            stay(u4, h).wait()
            back3(u4, h).wait()
            back4(u4, h).start()

    u3, on3 = at_step(J3)

    @pl.when(on3)
    def _():
        b = lax.rem(u3, SLOTS)
        for h in range(2):
            sum2(u3, h).wait()
            residual(u3, h).wait()
            total = keep2[b, h] + recv2[b, h].astype(jnp.float32) + res_s[b, h].astype(jnp.float32)
            fin_s[b, h] = total.astype(jnp.bfloat16)
            back3(u3, h).start()
            stay(u3, h).start()

    u2, on2 = at_step(J2)

    @pl.when(on2)
    def _():
        b = lax.rem(u2, SLOTS)
        for h in range(2):
            residual(u2, h).start()
            sum1(u2, h).wait()
            total = keep1[b, h] + recv1[b, h].astype(jnp.float32)
            send2[b, h] = total[:N].astype(jnp.bfloat16)
            keep2[b, h] = total[N:]
            sum2(u2, h).start()

    u1, on1 = at_step(J1)

    @pl.when(on1)
    def _():
        b = lax.rem(u1, SLOTS)
        sum0(u1).wait()
        for h in range(2):
            at = slice(h * 4 * N, (h + 1) * 4 * N)
            total = keep0[lax.rem(u1, 2), at] + recv0[b, at].astype(jnp.float32)
            send1[b, h] = total[: 2 * N].astype(jnp.bfloat16)
            keep1[b, h] = total[2 * N :]
            sum1(u1, h).start()

    u0, on0 = at_step(0)

    @pl.when(on0)
    def _():
        a = lax.rem(u0, 2)
        term = jnp.dot(seen_s[lax.rem(lax.div(u0, S), 2)], wo_ref[...], preferred_element_type=jnp.float32)
        send0[a] = term[: R // 2].astype(jnp.bfloat16)
        keep0[a] = term[R // 2 :]
        sum0(u0).start()

    pre = t < C

    @pl.when(pre & (n < R // RB))
    def _():
        def some(i, _):
            r = pl.multiple_of(i * 16, 16)
            wide = x_ref[pl.ds(r, 16), :].astype(jnp.float32)
            scale = lax.rsqrt(jnp.mean(wide * wide, -1, keepdims=True) + 1e-6)
            at = pl.multiple_of(n * RB + r, 16)
            normed_s[pl.ds(at, 16), :] = (wide * scale * gain_ref[...].astype(jnp.float32)).astype(jnp.bfloat16)

        lax.fori_loop(0, RB // 16, some, None)

    place = pl.ds(pl.multiple_of(t * R, R), R)

    @pl.when(pre & (n == R // RB))
    def _():
        @pl.when(t == 0)
        def _():
            for w in weights():
                w.wait()

        kv = jnp.dot(normed_s[...], wkv_s[...], preferred_element_type=jnp.float32).astype(jnp.bfloat16).astype(jnp.float32)
        k_s[place, :] = _turn(kv[:, :HEAD], table_ref[place, :])
        vt_s[:HEAD, place] = kv[:, HEAD:].T.astype(jnp.bfloat16)

    @pl.when(pre & (n > R // RB) & (n < S - 1))
    def _():
        q = jnp.dot(normed_s[...], wq_ref[...], preferred_element_type=jnp.float32).astype(jnp.bfloat16).astype(jnp.float32)
        table = table_ref[place, :]
        for i in range(2):
            q_s[i * R : (i + 1) * R, :] = _turn(q[:, i * HEAD : (i + 1) * HEAD], table)
        cols = 2 * R
        top_s[...] = jnp.full(top_s.shape, NEG, jnp.float32)
        mix_s[...] = jnp.zeros(mix_s.shape, jnp.float32)

        def block(j, masked):
            here = pl.ds(pl.multiple_of(j * BK, BK), BK)
            s = _dot(k_s[here, :], q_s[...], 1, 1)
            if masked:
                key = j * BK + lax.broadcasted_iota(jnp.int32, (BK, cols), 0)
                query = t * R + lax.rem(lax.broadcasted_iota(jnp.int32, (BK, cols), 1), R)
                s = jnp.where(key <= query, s, HIDDEN)
            old = top_s[0:1, :]
            top = jnp.maximum(old, s.max(axis=0, keepdims=True))
            top_s[0:1, :] = top
            p = jnp.exp2((s - top) * E).astype(jnp.bfloat16)
            mix_s[...] = mix_s[...] * jnp.exp2((old - top) * E) + _dot(vt_s[:, here], p, 1, 0)

        whole = lax.div(t * R, BK)
        lax.fori_loop(0, whole, lambda j, _: block(j, False), None)
        block(whole, True)
        out = (mix_s[:HEAD, :] * (1 / mix_s[HEAD : HEAD + 1, :])).T.astype(jnp.bfloat16)
        head = (n - R // RB - 1) * 2
        for p in range(16):
            c, h, b1, b2 = p >> 3, (p >> 2) & 1, (p >> 1) & 1, p & 1
            kept = lambda bit, mine: mine if bit else 1 - mine
            to = (kept(c, core) * 2 + h) * 4 + kept(b1, first[h]) * 2 + kept(b2, second[h])
            for i in range(2):
                at = pl.ds(pl.multiple_of((head + i) * HEAD, HEAD), HEAD)
                seen_s[lax.rem(t, 2), pl.ds(pl.multiple_of(to * N, N), N), at] = out[i * R + p * N : i * R + (p + 1) * N, :]


def _attention(x, gain, wq, wk, wv, wo):
    width = wq.shape[1]
    hbm = pl.BlockSpec(memory_space=pl.ANY)
    once = pl.Buffered(1)
    nb = R // RB
    div, rem = lax.div, lax.rem

    def q_block(g):
        i = rem(g, S) - nb - 1
        return 0, jnp.where((i >= 0) & (i < S - nb - 2) & (g < UNITS), i, 0)

    def wo_block(g):
        return 0, jnp.where(g < S, 0, jnp.where(g < S + UNITS, rem(g, S), S - 1))

    def x_block(g):
        ahead = jnp.where(rem(g, S) >= nb, div(g, S) * nb + nb, div(g, S) * nb + rem(g, S))
        return jnp.minimum(ahead, ROWS // RB - 1), 0

    bf, f32 = jnp.bfloat16, jnp.float32
    dma = pltpu.SemaphoreType.DMA
    return pl.pallas_call(
        _kernel,
        grid=(STEPS,),
        in_specs=[
            pl.BlockSpec((RB, D), x_block),
            pl.BlockSpec((1, D), lambda g: (0, 0), pipeline_mode=once),
            pl.BlockSpec((D, 2 * HEAD), q_block),
            pl.BlockSpec((width, BN), wo_block),
            pl.BlockSpec((ROWS, HEAD), lambda g: (0, 0), pipeline_mode=once),
            hbm, hbm, hbm,
        ],
        out_specs=hbm,
        out_shape=jax.ShapeDtypeStruct((ROWS, D), bf),
        scratch_shapes=[
            pltpu.VMEM((R, D), bf),
            pltpu.VMEM((D, 2 * HEAD), bf),
            pltpu.VMEM((ROWS, HEAD), bf),
            pltpu.VMEM((HEAD + 16, ROWS), bf),
            pltpu.VMEM((2, R, width), bf),
            pltpu.VMEM((2 * R, HEAD), bf),
            pltpu.VMEM((8, 2 * R), f32),
            pltpu.VMEM((HEAD + 16, 2 * R), f32),
            pltpu.VMEM((2, R // 2, BN), bf), pltpu.VMEM((2, R // 2, BN), f32), pltpu.VMEM((SLOTS, R // 2, BN), bf),
            pltpu.VMEM((SLOTS, 2, 2 * N, BN), bf), pltpu.VMEM((SLOTS, 2, 2 * N, BN), f32), pltpu.VMEM((SLOTS, 2, 2 * N, BN), bf),
            pltpu.VMEM((SLOTS, 2, N, BN), bf), pltpu.VMEM((SLOTS, 2, N, BN), f32), pltpu.VMEM((SLOTS, 2, N, BN), bf),
            pltpu.VMEM((SLOTS, 2, N, BN), bf), pltpu.VMEM((SLOTS, 2, N, BN), bf),
            dma((2,)),
            dma((SLOTS,)), dma((SLOTS,)), dma((SLOTS, 2)), dma((SLOTS, 2)), dma((SLOTS, 2)), dma((SLOTS, 2)),
            dma((SLOTS, 2)), dma((SLOTS, 2)), dma((SLOTS, 2)), dma((SLOTS, 2)), dma((SLOTS,)), dma((SLOTS,)),
            dma((SLOTS, 2)), dma((SLOTS, 2)),
        ],
        compiler_params=pltpu.CompilerParams(dimension_semantics=("arbitrary",), vmem_limit_bytes=64 * 2**20 - 65536, collective_id=0,
                                             has_side_effects=True),
        cost_estimate=pl.CostEstimate(flops=2 * ROWS * D * (2 * width + 2 * HEAD), transcendentals=0, bytes_accessed=C * 4 * D * width),
        name="layer",
    )(x, gain, wq, wo, _table(), x, wk, wv)


def solution(mesh):
    def step(x, gain, wq, wk, wv, wo):
        return _attention(x, gain.reshape(1, -1), wq, wk, wv, wo)

    tokens, columns = P("dp", None), P(None, "tp")
    return jax.shard_map(
        step,
        mesh=mesh,
        in_specs=(tokens, P(None), columns, columns, columns, P("tp", None)),
        out_specs=tokens,
        check_vma=False,
    )
```

```python
import functools

import jax
import jax.numpy as jnp
import numpy as np
from jax import lax
from jax.experimental import pallas as pl
from jax.experimental.pallas import tpu as pltpu
from jax.sharding import PartitionSpec as P

HEAD = 128
THETA = 10000
NEG = -1e30
HIDDEN = 2 * NEG
LOG2E = 1.4426950408889634
E = HEAD**-0.5 * LOG2E
ROWS, D = 2048, 12288
R = 256
S = 12
BN = D // S
RB = 64
BK = 512
C = ROWS // R
UNITS = C * S
N = R // 16
SLOTS = 8
J1, J2, J3, F4, F5, F6 = 1, 5, 9, 13, 17, 21
LATE = UNITS - S
STEPS = S + UNITS + F4
NB = R // RB
PAIRS = S - NB - 2


def _dot(a, b, ca, cb):
    return lax.dot_general(a, b, (((ca,), (cb,)), ((), ())), preferred_element_type=jnp.float32)


def _table():
    half = HEAD // 2
    freq = (np.float32(THETA) ** (-np.arange(half, dtype=np.float32) / np.float32(half))).astype(np.float32)
    angle = np.arange(ROWS, dtype=np.float32)[:, None] * freq
    return np.concatenate([np.cos(angle), np.sin(angle)], axis=1).astype(np.float32)


def _turn(t, table):
    half = HEAD // 2
    a, b, cos, sin = t[:, :half], t[:, half:], table[:, :half], table[:, half:]
    return jnp.concatenate([a * cos - b * sin, b * cos + a * sin], axis=1).astype(jnp.bfloat16)


def _kernel(x_ref, gain_ref, table_ref, x_hbm, wq_hbm, wk_hbm, wv_hbm, wo_hbm, y_hbm, late_a, late_b,
            normed_s, wkv_s, wq_s, wo_s, k_s, vt_s, seen_s, q_s, top_s, mix_s,
            send0, keep0, recv0, send1, keep1, recv1, send2, keep2, recv2, res_s, fin_s,
            w_sem, wq_sem, wo_sem, s0, r0, s1, r1, s2, r2, s3, r3, s4, r4, s5, r5, res_sem, fin_sem):
    g = pl.program_id(0)
    t, n = lax.div(g, S), lax.rem(g, S)
    me = lax.axis_index("tp")
    core, yb, xb = lax.rem(me, 2), lax.rem(lax.div(me, 2), 2), lax.div(me, 4)
    to_core, to_y, to_x = me + 1 - 2 * core, me + 2 - 4 * yb, me + 4 - 8 * xb
    first, second = (xb, yb), (yb, xb)
    to_first, to_second = (to_x, to_y), (to_y, to_x)

    def remote(src, dst, send_sem, recv_sem, to):
        return pltpu.make_async_remote_copy(src_ref=src, dst_ref=dst, send_sem=send_sem, recv_sem=recv_sem, device_id={"tp": to},
                                            device_id_type=pl.DeviceIdType.MESH)

    def rows_of(u, piece, count):
        row = pl.multiple_of(lax.div(u, S) * R + piece * N, N)
        return pl.ds(row, count * N), pl.ds(pl.multiple_of(lax.rem(u, S) * BN, BN), BN)

    def own(h):
        return core * 8 + h * 4 + first[h] * 2 + second[h]

    def weights():
        return [pltpu.make_async_copy(w, wkv_s.at[:, pl.ds(i * HEAD, HEAD)], w_sem.at[i]) for i, w in enumerate((wk_hbm, wv_hbm))]

    def queries(i):
        at = pl.ds(pl.multiple_of(i * 2 * HEAD, 2 * HEAD), 2 * HEAD)
        return pltpu.make_async_copy(wq_hbm.at[:, at], wq_s.at[lax.rem(i, 2)], wq_sem.at[lax.rem(i, 2)])

    def columns(u):
        at = pl.ds(pl.multiple_of(lax.rem(u, S) * BN, BN), BN)
        return pltpu.make_async_copy(wo_hbm.at[:, at], wo_s.at[lax.rem(u, 2)], wo_sem.at[lax.rem(u, 2)])

    def sum0(u):
        a, b = lax.rem(u, 2), lax.rem(u, SLOTS)
        return remote(send0.at[a], recv0.at[b], s0.at[b], r0.at[b], to_core)

    def sum1(u, h):
        b = lax.rem(u, SLOTS)
        return remote(send1.at[b, h], recv1.at[b, h], s1.at[b, h], r1.at[b, h], to_first[h])

    def sum2(u, h):
        b = lax.rem(u, SLOTS)
        return remote(send2.at[b, h], recv2.at[b, h], s2.at[b, h], r2.at[b, h], to_second[h])

    def residual(u, h):
        b = lax.rem(u, SLOTS)
        return pltpu.make_async_copy(x_hbm.at[rows_of(u, own(h), 1)], res_s.at[b, h], res_sem.at[b, h])

    def stay(u, h):
        b = lax.rem(u, SLOTS)
        return pltpu.make_async_copy(fin_s.at[b, h], y_hbm.at[rows_of(u, own(h), 1)], fin_sem.at[b, h])

    def late(u, h):
        row = pl.multiple_of(second[h] * N, N)
        return (late_a, late_b)[h].at[pl.ds(row, N), pl.ds(pl.multiple_of(lax.rem(u, S) * BN, BN), BN)]

    def stay_late(u, h):
        b = lax.rem(u, SLOTS)
        return pltpu.make_async_copy(fin_s.at[b, h], late(u, h), fin_sem.at[b, h])

    def back3(u, h):
        b = lax.rem(u, SLOTS)
        return remote(fin_s.at[b, h], y_hbm.at[rows_of(u, own(h), 1)], s3.at[b, h], r3.at[b, h], to_second[h])

    def back3_late(u, h):
        b = lax.rem(u, SLOTS)
        return remote(fin_s.at[b, h], late(u, h), s3.at[b, h], r3.at[b, h], to_second[h])

    def back4(u, h):
        b = lax.rem(u, SLOTS)
        at = rows_of(u, core * 8 + h * 4 + first[h] * 2, 2)
        return remote(y_hbm.at[at], y_hbm.at[at], s4.at[b, h], r4.at[b, h], to_first[h])

    def back5(u):
        b = lax.rem(u, SLOTS)
        at = rows_of(u, core * 8, 8)
        return remote(y_hbm.at[at], y_hbm.at[at], s5.at[b], r5.at[b], to_core)

    @pl.when(g == 0)
    def _():
        barrier = pltpu.get_barrier_semaphore()
        for to in (to_core, to_y, to_x):
            pl.semaphore_signal(barrier, inc=1, device_id={"tp": to}, device_id_type=pl.DeviceIdType.MESH)
        pl.semaphore_wait(barrier, 3)
        for w in weights():
            w.start()
        queries(0).start()
        k_s[...] = jnp.zeros_like(k_s)
        vt_s[...] = jnp.zeros_like(vt_s)
        vt_s[HEAD:, :] = jnp.ones((16, ROWS), vt_s.dtype)

    def at_step(lag):
        u = g - S - lag
        return u, (u >= 0) & (u < (LATE if lag > F4 else UNITS))

    ahead = g + 1 - S

    @pl.when((ahead >= 0) & (ahead < UNITS))
    def _():
        columns(ahead).start()

    u6, on6 = at_step(F6)

    @pl.when(on6)
    def _():
        back5(u6).wait()

    u5, on5 = at_step(F5)

    @pl.when(on5)
    def _():
        for h in range(2):
            back4(u5, h).wait()
        back5(u5).start()

    u4, on4 = at_step(F4)

    @pl.when(on4)
    def _():
        for h in range(2):
            stay(u4, h).wait()
            back3(u4, h).wait()

        @pl.when(u4 < LATE)
        def _():
            for h in range(2):
                back4(u4, h).start()

    u3, on3 = at_step(J3)

    @pl.when(on3)
    def _():
        b = lax.rem(u3, SLOTS)
        for h in range(2):
            sum2(u3, h).wait()
            residual(u3, h).wait()
            total = keep2[b, h] + recv2[b, h].astype(jnp.float32) + res_s[b, h].astype(jnp.float32)
            fin_s[b, h] = total.astype(jnp.bfloat16)

        @pl.when(u3 < LATE)
        def _():
            for h in range(2):
                back3(u3, h).start()
                stay(u3, h).start()

        @pl.when(u3 >= LATE)
        def _():
            for h in range(2):
                back3_late(u3, h).start()
                stay_late(u3, h).start()

    u2, on2 = at_step(J2)

    @pl.when(on2)
    def _():
        b = lax.rem(u2, SLOTS)
        for h in range(2):
            residual(u2, h).start()
            sum1(u2, h).wait()
            total = keep1[b, h] + recv1[b, h].astype(jnp.float32)
            send2[b, h] = total[:N].astype(jnp.bfloat16)
            keep2[b, h] = total[N:]
            sum2(u2, h).start()

    u1, on1 = at_step(J1)

    @pl.when(on1)
    def _():
        b = lax.rem(u1, SLOTS)
        sum0(u1).wait()
        for h in range(2):
            at = slice(h * 4 * N, (h + 1) * 4 * N)
            total = keep0[lax.rem(u1, 2), at] + recv0[b, at].astype(jnp.float32)
            send1[b, h] = total[: 2 * N].astype(jnp.bfloat16)
            keep1[b, h] = total[2 * N :]
            sum1(u1, h).start()

    u0, on0 = at_step(0)

    @pl.when(on0)
    def _():
        a = lax.rem(u0, 2)
        columns(u0).wait()
        term = jnp.dot(seen_s[lax.rem(lax.div(u0, S), 2)], wo_s[a], preferred_element_type=jnp.float32)
        send0[a] = term[: R // 2].astype(jnp.bfloat16)
        keep0[a] = term[R // 2 :]
        sum0(u0).start()

    pre = t < C

    @pl.when(pre & (n < NB))
    def _():
        for r in range(0, RB, 16):
            wide = x_ref[r : r + 16, :].astype(jnp.float32)
            scale = lax.rsqrt(jnp.mean(wide * wide, -1, keepdims=True) + 1e-6)
            at = pl.multiple_of(n * RB + r, 16)
            normed_s[pl.ds(at, 16), :] = (wide * scale * gain_ref[...].astype(jnp.float32)).astype(jnp.bfloat16)

    place = pl.ds(pl.multiple_of(t * R, R), R)

    @pl.when(pre & (n == NB))
    def _():
        @pl.when(t == 0)
        def _():
            for w in weights():
                w.wait()

        kv = jnp.dot(normed_s[...], wkv_s[...], preferred_element_type=jnp.float32).astype(jnp.bfloat16).astype(jnp.float32)
        k_s[place, :] = _turn(kv[:, :HEAD], table_ref[place, :])
        vt_s[:HEAD, place] = kv[:, HEAD:].T.astype(jnp.bfloat16)

    pair = n - NB - 1

    @pl.when((n == S - 1) & (t + 1 < C))
    def _():
        queries(0).start()

    @pl.when(pre & (pair >= 0) & (pair < PAIRS))
    def _():
        @pl.when(pair + 1 < PAIRS)
        def _():
            queries(pair + 1).start()

        queries(pair).wait()
        q = jnp.dot(normed_s[...], wq_s[lax.rem(pair, 2)], preferred_element_type=jnp.float32).astype(jnp.bfloat16).astype(jnp.float32)
        table = table_ref[place, :]
        for i in range(2):
            q_s[lax.rem(pair, 2), i * R : (i + 1) * R, :] = _turn(q[:, i * HEAD : (i + 1) * HEAD], table)

    @pl.when(pre & (pair >= 1))
    def _():
        q_ref = q_s.at[lax.rem(pair - 1, 2)]
        cols = 2 * R
        top_s[...] = jnp.full(top_s.shape, NEG, jnp.float32)
        mix_s[...] = jnp.zeros(mix_s.shape, jnp.float32)

        def block(first_key, bk, masked):
            here = pl.ds(pl.multiple_of(first_key, bk), bk)
            s = _dot(k_s[here, :], q_ref[...], 1, 1)
            if masked:
                key = first_key + lax.broadcasted_iota(jnp.int32, (bk, cols), 0)
                query = t * R + lax.rem(lax.broadcasted_iota(jnp.int32, (bk, cols), 1), R)
                s = jnp.where(key <= query, s, HIDDEN)
            old = top_s[0:1, :]
            top = jnp.maximum(old, s.max(axis=0, keepdims=True))
            top_s[0:1, :] = top
            p = jnp.exp2((s - top) * E).astype(jnp.bfloat16)
            mix_s[...] = mix_s[...] * jnp.exp2((old - top) * E) + _dot(vt_s[:, here], p, 1, 0)

        whole = lax.div(t * R, BK)
        lax.fori_loop(0, whole, lambda j, _: block(j * BK, BK, False), None)

        @pl.when(whole * BK < t * R)
        def _():
            block(whole * BK, BK, True)

        @pl.when(whole * BK == t * R)
        def _():
            block(t * R, R, True)

        out = (mix_s[:HEAD, :] * (1 / mix_s[HEAD : HEAD + 1, :])).T.astype(jnp.bfloat16)
        head = (pair - 1) * 2
        for p in range(16):
            c, h, b1, b2 = p >> 3, (p >> 2) & 1, (p >> 1) & 1, p & 1
            kept = lambda bit, mine: mine if bit else 1 - mine
            to = (kept(c, core) * 2 + h) * 4 + kept(b1, first[h]) * 2 + kept(b2, second[h])
            for i in range(2):
                at = pl.ds(pl.multiple_of((head + i) * HEAD, HEAD), HEAD)
                seen_s[lax.rem(t, 2), pl.ds(pl.multiple_of(to * N, N), N), at] = out[i * R + p * N : i * R + (p + 1) * N, :]


def _attention(x, gain, wq, wk, wv, wo):
    width = wq.shape[1]
    hbm = pl.BlockSpec(memory_space=pl.ANY)
    once = pl.Buffered(1)
    div, rem = lax.div, lax.rem

    def x_block(g):
        ahead = jnp.where(rem(g, S) >= NB, div(g, S) * NB + NB, div(g, S) * NB + rem(g, S))
        return jnp.minimum(ahead, ROWS // RB - 1), 0

    bf, f32 = jnp.bfloat16, jnp.float32
    dma = pltpu.SemaphoreType.DMA
    return pl.pallas_call(
        _kernel,
        grid=(STEPS,),
        in_specs=[
            pl.BlockSpec((RB, D), x_block),
            pl.BlockSpec((1, D), lambda g: (0, 0), pipeline_mode=once),
            pl.BlockSpec((ROWS, HEAD), lambda g: (0, 0), pipeline_mode=once),
            hbm, hbm, hbm, hbm, hbm,
        ],
        out_specs=[hbm] * 3,
        out_shape=[jax.ShapeDtypeStruct((n, D), bf) for n in (ROWS, 2 * N, 2 * N)],
        scratch_shapes=[
            pltpu.VMEM((R, D), bf),
            pltpu.VMEM((D, 2 * HEAD), bf),
            pltpu.VMEM((2, D, 2 * HEAD), bf),
            pltpu.VMEM((2, width, BN), bf),
            pltpu.VMEM((ROWS, HEAD), bf),
            pltpu.VMEM((HEAD + 16, ROWS), bf),
            pltpu.VMEM((2, R, width), bf),
            pltpu.VMEM((2, 2 * R, HEAD), bf),
            pltpu.VMEM((8, 2 * R), f32),
            pltpu.VMEM((HEAD + 16, 2 * R), f32),
            pltpu.VMEM((2, R // 2, BN), bf), pltpu.VMEM((2, R // 2, BN), f32), pltpu.VMEM((SLOTS, R // 2, BN), bf),
            pltpu.VMEM((SLOTS, 2, 2 * N, BN), bf), pltpu.VMEM((SLOTS, 2, 2 * N, BN), f32), pltpu.VMEM((SLOTS, 2, 2 * N, BN), bf),
            pltpu.VMEM((SLOTS, 2, N, BN), bf), pltpu.VMEM((SLOTS, 2, N, BN), f32), pltpu.VMEM((SLOTS, 2, N, BN), bf),
            pltpu.VMEM((SLOTS, 2, N, BN), bf), pltpu.VMEM((SLOTS, 2, N, BN), bf),
            dma((2,)), dma((2,)), dma((2,)),
            dma((SLOTS,)), dma((SLOTS,)), dma((SLOTS, 2)), dma((SLOTS, 2)), dma((SLOTS, 2)), dma((SLOTS, 2)),
            dma((SLOTS, 2)), dma((SLOTS, 2)), dma((SLOTS, 2)), dma((SLOTS, 2)), dma((SLOTS,)), dma((SLOTS,)),
            dma((SLOTS, 2)), dma((SLOTS, 2)),
        ],
        compiler_params=pltpu.CompilerParams(dimension_semantics=("arbitrary",), vmem_limit_bytes=64 * 2**20 - 65536, collective_id=0,
                                             has_side_effects=True),
        cost_estimate=pl.CostEstimate(flops=2 * ROWS * D * (2 * width + 2 * HEAD), transcendentals=0, bytes_accessed=C * 4 * D * width),
        name="layer",
    )(x, gain, _table(), x, wq, wk, wv, wo)


def _move_kernel(blocks, src_ref, *rest):
    dst_ref, buf, in_sem, out_sem = rest[-4:]
    ring, rb = buf.shape[0], buf.shape[1]
    at = lambda i: pl.ds(blocks[i] * rb, rb)
    get = lambda i: pltpu.make_async_copy(src_ref.at[at(i)], buf.at[i % ring], in_sem.at[i % ring])
    put = lambda i: pltpu.make_async_copy(buf.at[i % ring], dst_ref.at[at(i)], out_sem.at[i % ring])
    count, lag = len(blocks), ring // 2
    for i in range(count + lag):
        if i < count:
            if i >= ring:
                put(i - ring).wait()
            get(i).start()
        if i >= lag:
            get(i - lag).wait()
            put(i - lag).start()
    for i in range(max(count - ring, 0), count):
        put(i).wait()


def _move(src, dst, row0, row1):
    rb, ring = 64, 12
    hbm = pl.BlockSpec(memory_space=pl.ANY)
    args = (src,) if dst is None else (src, dst)
    return pl.pallas_call(
        functools.partial(_move_kernel, tuple(range(row0 // rb, row1 // rb))),
        in_specs=[hbm] * len(args),
        out_specs=hbm,
        out_shape=jax.ShapeDtypeStruct((ROWS, D), jnp.bfloat16),
        scratch_shapes=[pltpu.VMEM((ring, rb, D), jnp.bfloat16), pltpu.SemaphoreType.DMA((ring,)), pltpu.SemaphoreType.DMA((ring,))],
        input_output_aliases={} if dst is None else {1: 0},
        compiler_params=pltpu.CompilerParams(vmem_limit_bytes=48 * 2**20),
        cost_estimate=pl.CostEstimate(flops=(row1 - row0) * D * 2000, transcendentals=0, bytes_accessed=(row1 - row0) * D * 4),
        name="move",
    )(*args)


def _place_kernel(row0, n, *refs):
    pieces, (y_ref, buf, in_sem, out_sem) = refs[:8], refs[-4:]
    me = lax.axis_index("tp")
    core, yb, xb = lax.rem(me, 2), lax.rem(lax.div(me, 2), 2), lax.div(me, 4)
    gets, puts = [], []
    for i, piece in enumerate(pieces):
        c, h, p1 = (1 - core if i >= 4 else core), i % 2, (xb, yb)[i % 2]
        p1 = 1 - p1 if i % 4 >= 2 else p1
        at = pl.multiple_of(row0 + (c * 4 + h * 2 + p1) * n, n)
        gets.append(pltpu.make_async_copy(piece, buf.at[i], in_sem.at[i]))
        puts.append(pltpu.make_async_copy(buf.at[i], y_ref.at[pl.ds(at, n)], out_sem.at[i]))
    for get in gets:
        get.start()
    for get, put in zip(gets, puts):
        get.wait()
        put.start()
    for put in puts:
        put.wait()


def _place(pieces, y):
    n = pieces[0].shape[0]
    hbm = pl.BlockSpec(memory_space=pl.ANY)
    return pl.pallas_call(
        functools.partial(_place_kernel, ROWS - R, n),
        in_specs=[hbm] * 9,
        out_specs=hbm,
        out_shape=jax.ShapeDtypeStruct((ROWS, D), jnp.bfloat16),
        scratch_shapes=[pltpu.VMEM((8, n, D), jnp.bfloat16), pltpu.SemaphoreType.DMA((8,)), pltpu.SemaphoreType.DMA((8,))],
        input_output_aliases={8: 0},
        compiler_params=pltpu.CompilerParams(vmem_limit_bytes=48 * 2**20),
        cost_estimate=pl.CostEstimate(flops=R * D * 100, transcendentals=0, bytes_accessed=R * D * 4),
        name="place",
    )(*pieces, y)


def solution(mesh):
    def swap(t, bit):
        return lax.ppermute(t, "tp", [(i, i ^ bit) for i in range(8)])

    def step(x, gain, wq, wk, wv, wo):
        y, late_a, late_b = _attention(x, gain.reshape(1, -1), wq, wk, wv, wo)
        own = [late_a, late_b]
        along = [swap(late_a, 4), swap(late_b, 2)]
        other = [swap(t, 1) for t in own]
        cut = (ROWS - R) // 128 * 72
        done = _move(y, None, 0, cut)
        along, done = lax.optimization_barrier((along, done))
        done = _move(y, done, cut, ROWS - R)
        other += [swap(t, 1) for t in along]
        return _place(own + along + other, done)

    tokens, columns = P("dp", None), P(None, "tp")
    return jax.shard_map(
        step,
        mesh=mesh,
        in_specs=(tokens, P(None), columns, columns, columns, P("tp", None)),
        out_specs=tokens,
        check_vma=False,
    )
```

```python
import functools

import jax
import jax.numpy as jnp
import numpy as np
from jax import lax
from jax.experimental import pallas as pl
from jax.experimental.pallas import tpu as pltpu
from jax.sharding import PartitionSpec as P

HEAD = 128
THETA = 10000
NEG = -1e30
HIDDEN = 2 * NEG
LOG2E = 1.4426950408889634
E = HEAD**-0.5 * LOG2E
ROWS, D = 2048, 12288
R = 256
S = 12
BN = D // S
RB = 64
BK = 512
C = ROWS // R
UNITS = C * S
N = R // 16
SLOTS = 8
J1, J2, J3, F4, F5, F6 = 1, 5, 9, 13, 17, 21
TAIL = 2
LATE = UNITS - TAIL * S
STEPS = S + UNITS + F4
NB = R // RB
PAIRS = S - NB - 2


def _dot(a, b, ca, cb):
    return lax.dot_general(a, b, (((ca,), (cb,)), ((), ())), preferred_element_type=jnp.float32)


def _table():
    half = HEAD // 2
    freq = (np.float32(THETA) ** (-np.arange(half, dtype=np.float32) / np.float32(half))).astype(np.float32)
    angle = np.arange(ROWS, dtype=np.float32)[:, None] * freq
    return np.concatenate([np.cos(angle), np.sin(angle)], axis=1).astype(np.float32)


def _turn(t, table):
    half = HEAD // 2
    a, b, cos, sin = t[:, :half], t[:, half:], table[:, :half], table[:, half:]
    return jnp.concatenate([a * cos - b * sin, b * cos + a * sin], axis=1).astype(jnp.bfloat16)


def _kernel(x_ref, gain_ref, table_ref, x_hbm, wq_hbm, wk_hbm, wv_hbm, wo_hbm, y_hbm, *rest):
    lates, rest = rest[: 2 * TAIL], rest[2 * TAIL :]
    (normed_s, wkv_s, wq_s, wo_s, k_s, vt_s, seen_s, q_s, top_s, mix_s,
     send0, keep0, recv0, send1, keep1, recv1, send2, keep2, recv2, res_s, fin_s,
     w_sem, wq_sem, wo_sem, s0, r0, s1, r1, s2, r2, s3, r3, s4, r4, s5, r5, res_sem, fin_sem) = rest
    g = pl.program_id(0)
    t, n = lax.div(g, S), lax.rem(g, S)
    me = lax.axis_index("tp")
    core, yb, xb = lax.rem(me, 2), lax.rem(lax.div(me, 2), 2), lax.div(me, 4)
    to_core, to_y, to_x = me + 1 - 2 * core, me + 2 - 4 * yb, me + 4 - 8 * xb
    first, second = (xb, yb), (yb, xb)
    to_first, to_second = (to_x, to_y), (to_y, to_x)

    def remote(src, dst, send_sem, recv_sem, to):
        return pltpu.make_async_remote_copy(src_ref=src, dst_ref=dst, send_sem=send_sem, recv_sem=recv_sem, device_id={"tp": to},
                                            device_id_type=pl.DeviceIdType.MESH)

    def rows_of(u, piece, count):
        row = pl.multiple_of(lax.div(u, S) * R + piece * N, N)
        return pl.ds(row, count * N), pl.ds(pl.multiple_of(lax.rem(u, S) * BN, BN), BN)

    def own(h):
        return core * 8 + h * 4 + first[h] * 2 + second[h]

    def weights():
        return [pltpu.make_async_copy(w, wkv_s.at[:, pl.ds(i * HEAD, HEAD)], w_sem.at[i]) for i, w in enumerate((wk_hbm, wv_hbm))]

    def queries(i):
        at = pl.ds(pl.multiple_of(i * 2 * HEAD, 2 * HEAD), 2 * HEAD)
        return pltpu.make_async_copy(wq_hbm.at[:, at], wq_s.at[lax.rem(i, 2)], wq_sem.at[lax.rem(i, 2)])

    def columns(u):
        at = pl.ds(pl.multiple_of(lax.rem(u, S) * BN, BN), BN)
        return pltpu.make_async_copy(wo_hbm.at[:, at], wo_s.at[lax.rem(u, 2)], wo_sem.at[lax.rem(u, 2)])

    def sum0(u):
        a, b = lax.rem(u, 2), lax.rem(u, SLOTS)
        return remote(send0.at[a], recv0.at[b], s0.at[b], r0.at[b], to_core)

    def sum1(u, h):
        b = lax.rem(u, SLOTS)
        return remote(send1.at[b, h], recv1.at[b, h], s1.at[b, h], r1.at[b, h], to_first[h])

    def sum2(u, h):
        b = lax.rem(u, SLOTS)
        return remote(send2.at[b, h], recv2.at[b, h], s2.at[b, h], r2.at[b, h], to_second[h])

    def residual(u, h):
        b = lax.rem(u, SLOTS)
        return pltpu.make_async_copy(x_hbm.at[rows_of(u, own(h), 1)], res_s.at[b, h], res_sem.at[b, h])

    def stay(u, h):
        b = lax.rem(u, SLOTS)
        return pltpu.make_async_copy(fin_s.at[b, h], y_hbm.at[rows_of(u, own(h), 1)], fin_sem.at[b, h])

    def late(u, h, i):
        row = pl.multiple_of(second[h] * N, N)
        return lates[2 * i + h].at[pl.ds(row, N), pl.ds(pl.multiple_of(lax.rem(u, S) * BN, BN), BN)]

    def stay_late(u, h, i):
        b = lax.rem(u, SLOTS)
        return pltpu.make_async_copy(fin_s.at[b, h], late(u, h, i), fin_sem.at[b, h])

    def back3(u, h):
        b = lax.rem(u, SLOTS)
        return remote(fin_s.at[b, h], y_hbm.at[rows_of(u, own(h), 1)], s3.at[b, h], r3.at[b, h], to_second[h])

    def back3_late(u, h, i):
        b = lax.rem(u, SLOTS)
        return remote(fin_s.at[b, h], late(u, h, i), s3.at[b, h], r3.at[b, h], to_second[h])

    def back4(u, h):
        b = lax.rem(u, SLOTS)
        at = rows_of(u, core * 8 + h * 4 + first[h] * 2, 2)
        return remote(y_hbm.at[at], y_hbm.at[at], s4.at[b, h], r4.at[b, h], to_first[h])

    def back5(u):
        b = lax.rem(u, SLOTS)
        at = rows_of(u, core * 8, 8)
        return remote(y_hbm.at[at], y_hbm.at[at], s5.at[b], r5.at[b], to_core)

    @pl.when(g == 0)
    def _():
        barrier = pltpu.get_barrier_semaphore()
        for to in (to_core, to_y, to_x):
            pl.semaphore_signal(barrier, inc=1, device_id={"tp": to}, device_id_type=pl.DeviceIdType.MESH)
        for w in weights():
            w.start()
        queries(0).start()
        k_s[...] = jnp.zeros_like(k_s)
        vt_s[...] = jnp.zeros_like(vt_s)
        vt_s[HEAD:, :] = jnp.ones((16, ROWS), vt_s.dtype)

    @pl.when(g == S - 1)
    def _():
        pl.semaphore_wait(pltpu.get_barrier_semaphore(), 3)

    def at_step(lag):
        u = g - S - lag
        return u, (u >= 0) & (u < (LATE if lag > F4 else UNITS))

    ahead = g + 1 - S

    @pl.when((ahead >= 0) & (ahead < UNITS))
    def _():
        columns(ahead).start()

    u6, on6 = at_step(F6)

    @pl.when(on6)
    def _():
        back5(u6).wait()

    u5, on5 = at_step(F5)

    @pl.when(on5)
    def _():
        for h in range(2):
            back4(u5, h).wait()
        back5(u5).start()

    u4, on4 = at_step(F4)

    @pl.when(on4)
    def _():
        for h in range(2):
            stay(u4, h).wait()
            back3(u4, h).wait()

        @pl.when(u4 < LATE)
        def _():
            for h in range(2):
                back4(u4, h).start()

    u3, on3 = at_step(J3)

    @pl.when(on3)
    def _():
        b = lax.rem(u3, SLOTS)
        for h in range(2):
            sum2(u3, h).wait()
            residual(u3, h).wait()
            total = keep2[b, h] + recv2[b, h].astype(jnp.float32) + res_s[b, h].astype(jnp.float32)
            fin_s[b, h] = total.astype(jnp.bfloat16)

        @pl.when(u3 < LATE)
        def _():
            for h in range(2):
                back3(u3, h).start()
                stay(u3, h).start()

        for i in range(TAIL):

            @pl.when(lax.div(u3, S) == C - TAIL + i)
            def _():
                for h in range(2):
                    back3_late(u3, h, i).start()
                    stay_late(u3, h, i).start()

    u2, on2 = at_step(J2)

    @pl.when(on2)
    def _():
        b = lax.rem(u2, SLOTS)
        for h in range(2):
            residual(u2, h).start()
            sum1(u2, h).wait()
            total = keep1[b, h] + recv1[b, h].astype(jnp.float32)
            send2[b, h] = total[:N].astype(jnp.bfloat16)
            keep2[b, h] = total[N:]
            sum2(u2, h).start()

    u1, on1 = at_step(J1)

    @pl.when(on1)
    def _():
        b = lax.rem(u1, SLOTS)
        sum0(u1).wait()
        for h in range(2):
            at = slice(h * 4 * N, (h + 1) * 4 * N)
            total = keep0[lax.rem(u1, 2), at] + recv0[b, at].astype(jnp.float32)
            send1[b, h] = total[: 2 * N].astype(jnp.bfloat16)
            keep1[b, h] = total[2 * N :]
            sum1(u1, h).start()

    u0, on0 = at_step(0)

    @pl.when(on0)
    def _():
        a = lax.rem(u0, 2)
        columns(u0).wait()
        term = jnp.dot(seen_s[lax.rem(lax.div(u0, S), 2)], wo_s[a], preferred_element_type=jnp.float32)
        send0[a] = term[: R // 2].astype(jnp.bfloat16)
        keep0[a] = term[R // 2 :]
        sum0(u0).start()

    pre = t < C

    @pl.when(pre & (n < NB))
    def _():
        groups, width = range(0, RB, 16), 1024
        scales = []
        for r in groups:
            squares = jnp.zeros((16, width), jnp.float32)
            for c in range(0, D, width):
                wide = x_ref[r : r + 16, c : c + width].astype(jnp.float32)
                squares += wide * wide
            scales.append(lax.rsqrt(jnp.sum(squares, -1, keepdims=True) * (1 / D) + 1e-6))
        for c in range(0, D, width):
            gain = gain_ref[c : c + width].astype(jnp.float32)[None, :]
            for r, scale in zip(groups, scales):
                at = pl.multiple_of(n * RB + r, 16)
                wide = x_ref[r : r + 16, c : c + width].astype(jnp.float32)
                normed_s[pl.ds(at, 16), c : c + width] = (wide * scale * gain).astype(jnp.bfloat16)

    place = pl.ds(pl.multiple_of(t * R, R), R)

    @pl.when(pre & (n == NB))
    def _():
        @pl.when(t == 0)
        def _():
            for w in weights():
                w.wait()

        kv = jnp.dot(normed_s[...], wkv_s[...], preferred_element_type=jnp.float32).astype(jnp.bfloat16).astype(jnp.float32)
        k_s[place, :] = _turn(kv[:, :HEAD], table_ref[place, :])
        vt_s[:HEAD, place] = kv[:, HEAD:].T.astype(jnp.bfloat16)

    pair = n - NB - 1

    @pl.when((n == S - 1) & (t + 1 < C))
    def _():
        queries(0).start()

    @pl.when(pre & (pair >= 0) & (pair < PAIRS))
    def _():
        @pl.when(pair + 1 < PAIRS)
        def _():
            queries(pair + 1).start()

        queries(pair).wait()
        q = jnp.dot(normed_s[...], wq_s[lax.rem(pair, 2)], preferred_element_type=jnp.float32).astype(jnp.bfloat16).astype(jnp.float32)
        table = table_ref[place, :]
        for i in range(2):
            q_s[lax.rem(pair, 2), i * R : (i + 1) * R, :] = _turn(q[:, i * HEAD : (i + 1) * HEAD], table)

    @pl.when(pre & (pair >= 1))
    def _():
        q_ref = q_s.at[lax.rem(pair - 1, 2)]
        cols = 2 * R
        top_s[...] = jnp.full(top_s.shape, NEG, jnp.float32)
        mix_s[...] = jnp.zeros(mix_s.shape, jnp.float32)

        def block(first_key, bk, masked):
            here = pl.ds(pl.multiple_of(first_key, bk), bk)
            s = _dot(k_s[here, :], q_ref[...], 1, 1)
            if masked:
                key = first_key + lax.broadcasted_iota(jnp.int32, (bk, cols), 0)
                query = t * R + lax.rem(lax.broadcasted_iota(jnp.int32, (bk, cols), 1), R)
                s = jnp.where(key <= query, s, HIDDEN)
            old = top_s[0:1, :]
            top = jnp.maximum(old, s.max(axis=0, keepdims=True))
            top_s[0:1, :] = top
            p = jnp.exp2((s - top) * E).astype(jnp.bfloat16)
            mix_s[...] = mix_s[...] * jnp.exp2((old - top) * E) + _dot(vt_s[:, here], p, 1, 0)

        whole = lax.div(t * R, BK)
        lax.fori_loop(0, whole, lambda j, _: block(j * BK, BK, False), None)

        @pl.when(whole * BK < t * R)
        def _():
            block(whole * BK, BK, True)

        @pl.when(whole * BK == t * R)
        def _():
            block(t * R, R, True)

        out = (mix_s[:HEAD, :] * (1 / mix_s[HEAD : HEAD + 1, :])).T.astype(jnp.bfloat16)
        head = (pair - 1) * 2
        for p in range(16):
            c, h, b1, b2 = p >> 3, (p >> 2) & 1, (p >> 1) & 1, p & 1
            kept = lambda bit, mine: mine if bit else 1 - mine
            to = (kept(c, core) * 2 + h) * 4 + kept(b1, first[h]) * 2 + kept(b2, second[h])
            for i in range(2):
                at = pl.ds(pl.multiple_of((head + i) * HEAD, HEAD), HEAD)
                seen_s[lax.rem(t, 2), pl.ds(pl.multiple_of(to * N, N), N), at] = out[i * R + p * N : i * R + (p + 1) * N, :]


def _attention(x, gain, wq, wk, wv, wo):
    width = wq.shape[1]
    hbm = pl.BlockSpec(memory_space=pl.ANY)
    once = pl.Buffered(1)
    div, rem = lax.div, lax.rem

    def x_block(g):
        ahead = jnp.where(rem(g, S) >= NB, div(g, S) * NB + NB, div(g, S) * NB + rem(g, S))
        return jnp.minimum(ahead, ROWS // RB - 1), 0

    bf, f32 = jnp.bfloat16, jnp.float32
    dma = pltpu.SemaphoreType.DMA
    return pl.pallas_call(
        _kernel,
        grid=(STEPS,),
        in_specs=[
            pl.BlockSpec((RB, D), x_block),
            pl.BlockSpec((D,), lambda g: (0,), pipeline_mode=once),
            pl.BlockSpec((ROWS, HEAD), lambda g: (0, 0), pipeline_mode=once),
            hbm, hbm, hbm, hbm, hbm,
        ],
        out_specs=[hbm] * (1 + 2 * TAIL),
        out_shape=[jax.ShapeDtypeStruct((n, D), bf) for n in (ROWS, *[2 * N] * (2 * TAIL))],
        scratch_shapes=[
            pltpu.VMEM((R, D), bf),
            pltpu.VMEM((D, 2 * HEAD), bf),
            pltpu.VMEM((2, D, 2 * HEAD), bf),
            pltpu.VMEM((2, width, BN), bf),
            pltpu.VMEM((ROWS, HEAD), bf),
            pltpu.VMEM((HEAD + 16, ROWS), bf),
            pltpu.VMEM((2, R, width), bf),
            pltpu.VMEM((2, 2 * R, HEAD), bf),
            pltpu.VMEM((8, 2 * R), f32),
            pltpu.VMEM((HEAD + 16, 2 * R), f32),
            pltpu.VMEM((2, R // 2, BN), bf), pltpu.VMEM((2, R // 2, BN), f32), pltpu.VMEM((SLOTS, R // 2, BN), bf),
            pltpu.VMEM((SLOTS, 2, 2 * N, BN), bf), pltpu.VMEM((SLOTS, 2, 2 * N, BN), f32), pltpu.VMEM((SLOTS, 2, 2 * N, BN), bf),
            pltpu.VMEM((SLOTS, 2, N, BN), bf), pltpu.VMEM((SLOTS, 2, N, BN), f32), pltpu.VMEM((SLOTS, 2, N, BN), bf),
            pltpu.VMEM((SLOTS, 2, N, BN), bf), pltpu.VMEM((SLOTS, 2, N, BN), bf),
            dma((2,)), dma((2,)), dma((2,)),
            dma((SLOTS,)), dma((SLOTS,)), dma((SLOTS, 2)), dma((SLOTS, 2)), dma((SLOTS, 2)), dma((SLOTS, 2)),
            dma((SLOTS, 2)), dma((SLOTS, 2)), dma((SLOTS, 2)), dma((SLOTS, 2)), dma((SLOTS,)), dma((SLOTS,)),
            dma((SLOTS, 2)), dma((SLOTS, 2)),
        ],
        compiler_params=pltpu.CompilerParams(dimension_semantics=("arbitrary",), vmem_limit_bytes=64 * 2**20 - 65536, collective_id=0,
                                             has_side_effects=True),
        cost_estimate=pl.CostEstimate(flops=2 * ROWS * D * (2 * width + 2 * HEAD), transcendentals=0, bytes_accessed=C * 4 * D * width),
        name="layer",
    )(x, gain, _table(), x, wq, wk, wv, wo)


def _move_kernel(blocks, src_ref, *rest):
    dst_ref, buf, in_sem, out_sem = rest[-4:]
    ring, rb = buf.shape[0], buf.shape[1]
    at = lambda i: pl.ds(blocks[i] * rb, rb)
    get = lambda i: pltpu.make_async_copy(src_ref.at[at(i)], buf.at[i % ring], in_sem.at[i % ring])
    put = lambda i: pltpu.make_async_copy(buf.at[i % ring], dst_ref.at[at(i)], out_sem.at[i % ring])
    count, lag = len(blocks), ring // 2
    for i in range(count + lag):
        if i < count:
            if i >= ring:
                put(i - ring).wait()
            get(i).start()
        if i >= lag:
            get(i - lag).wait()
            put(i - lag).start()
    for i in range(max(count - ring, 0), count):
        put(i).wait()


def _move(src, dst, row0, row1):
    rb, ring = 64, 12
    hbm = pl.BlockSpec(memory_space=pl.ANY)
    args = (src,) if dst is None else (src, dst)
    return pl.pallas_call(
        functools.partial(_move_kernel, tuple(range(row0 // rb, row1 // rb))),
        in_specs=[hbm] * len(args),
        out_specs=hbm,
        out_shape=jax.ShapeDtypeStruct((ROWS, D), jnp.bfloat16),
        scratch_shapes=[pltpu.VMEM((ring, rb, D), jnp.bfloat16), pltpu.SemaphoreType.DMA((ring,)), pltpu.SemaphoreType.DMA((ring,))],
        input_output_aliases={} if dst is None else {1: 0},
        compiler_params=pltpu.CompilerParams(vmem_limit_bytes=48 * 2**20),
        cost_estimate=pl.CostEstimate(flops=(row1 - row0) * D * 2000, transcendentals=0, bytes_accessed=(row1 - row0) * D * 4),
        name="move",
    )(*args)


def _place_kernel(where, *refs):
    pieces, (y_ref, buf, in_sem, out_sem) = refs[: len(where)], refs[-4:]
    me = lax.axis_index("tp")
    core, yb, xb = lax.rem(me, 2), lax.rem(lax.div(me, 2), 2), lax.div(me, 4)
    gets, puts = [], []
    for i, (piece, (row0, other, h, moved)) in enumerate(zip(pieces, where)):
        n = piece.shape[0]
        c = 1 - core if other else core
        p1 = (xb, yb)[h]
        p1 = 1 - p1 if moved else p1
        at = pl.multiple_of(row0 + (c * 4 + h * 2 + p1) * n, n)
        gets.append(pltpu.make_async_copy(piece, buf.at[i], in_sem.at[i]))
        puts.append(pltpu.make_async_copy(buf.at[i], y_ref.at[pl.ds(at, n)], out_sem.at[i]))
    for get in gets:
        get.start()
    for get, put in zip(gets, puts):
        get.wait()
        put.start()
    for put in puts:
        put.wait()


def _place(items, y):
    where, pieces = zip(*items)
    count, n = len(pieces), pieces[0].shape[0]
    hbm = pl.BlockSpec(memory_space=pl.ANY)
    return pl.pallas_call(
        functools.partial(_place_kernel, where),
        in_specs=[hbm] * (count + 1),
        out_specs=hbm,
        out_shape=jax.ShapeDtypeStruct((ROWS, D), jnp.bfloat16),
        scratch_shapes=[pltpu.VMEM((count, n, D), jnp.bfloat16), pltpu.SemaphoreType.DMA((count,)), pltpu.SemaphoreType.DMA((count,))],
        input_output_aliases={count: 0},
        compiler_params=pltpu.CompilerParams(vmem_limit_bytes=32 * 2**20),
        cost_estimate=pl.CostEstimate(flops=count * n * D * 2000, transcendentals=0, bytes_accessed=count * n * D * 4),
        name="place",
    )(*pieces, y)


def solution(mesh):
    def swap(t, bit):
        return lax.ppermute(t, "tp", [(i, i ^ bit) for i in range(8)])

    def step(x, gain, wq, wk, wv, wo):
        y, *lates = _attention(x, gain, wq, wk, wv, wo)
        owns = [lates[2 * i : 2 * i + 2] for i in range(TAIL)]
        alongs = [[swap(a, 4), swap(b, 2)] for a, b in owns]
        others = [[swap(a, 1), swap(b, 1)] for a, b in owns]
        rows = [ROWS - (TAIL - i) * R for i in range(TAIL)]
        ends = [0, 14 * RB, ROWS - TAIL * R]
        done, ready = None, []
        for i in range(TAIL):
            done = _move(y, done, ends[i], ends[i + 1])
            for h in range(2):
                ready += [((rows[i], 0, h, 0), owns[i][h]), ((rows[i], 1, h, 0), others[i][h])]
            if i < TAIL - 1:
                alongs[i], done = lax.optimization_barrier((alongs[i], done))
                for h in range(2):
                    ready += [((rows[i], 0, h, 1), alongs[i][h]), ((rows[i], 1, h, 1), swap(alongs[i][h], 1))]
        done = _place(ready, done)
        last, done = lax.optimization_barrier((alongs[-1], done))
        far = [swap(t, 1) for t in last]
        done = _place([((rows[-1], 0, h, 1), last[h]) for h in range(2)], done)
        far, done = lax.optimization_barrier((far, done))
        return _place([((rows[-1], 1, h, 1), far[h]) for h in range(2)], done)

    tokens, columns = P("dp", None), P(None, "tp")
    return jax.shard_map(
        step,
        mesh=mesh,
        in_specs=(tokens, P(None), columns, columns, columns, P("tp", None)),
        out_specs=tokens,
        check_vma=False,
    )
```

```python
import functools

import jax
import jax.numpy as jnp
import numpy as np
from jax import lax
from jax.experimental import pallas as pl
from jax.experimental.pallas import tpu as pltpu
from jax.sharding import PartitionSpec as P

HEAD = 128
THETA = 10000
NEG = -1e30
HIDDEN = 2 * NEG
LOG2E = 1.4426950408889634
E = HEAD**-0.5 * LOG2E
ROWS, D = 2048, 12288
R = 256
S = 12
BN = D // S
RB = 64
BK = 512
C = ROWS // R
UNITS = C * S
N = R // 16
SLOTS = 8
J1, J2, J3, F4, F5, F6 = range(6)
WAITS = ((2, 0, 8), (3, 8, 20), (4, 20, UNITS))
TAIL = 2
LATE = UNITS - TAIL * S
STEPS = S + UNITS + 1 + WAITS[-1][0] * F4
NB = R // RB
PAIRS = S - NB - 2


def _dot(a, b, ca, cb):
    return lax.dot_general(a, b, (((ca,), (cb,)), ((), ())), preferred_element_type=jnp.float32)


def _table():
    half = HEAD // 2
    freq = (np.float32(THETA) ** (-np.arange(half, dtype=np.float32) / np.float32(half))).astype(np.float32)
    angle = np.arange(ROWS, dtype=np.float32)[:, None] * freq
    return np.concatenate([np.cos(angle), np.sin(angle)], axis=1).astype(np.float32)


def _turn(t, cos, sin):
    return (t * cos + pltpu.roll(t, HEAD // 2, 1) * sin).astype(jnp.bfloat16)


def _kernel(x_ref, gain_ref, table_ref, x_hbm, wq_hbm, wk_hbm, wv_hbm, wo_hbm, y_hbm, *rest):
    lates, rest = rest[: 2 * TAIL], rest[2 * TAIL :]
    (normed_s, wkv_s, wq_s, wo_s, k_s, vt_s, seen_s, turn_s, q_s, top_s, mix_s,
     send0, keep0, recv0, send1, keep1, recv1, send2, keep2, recv2, res_s, fin_s,
     w_sem, wq_sem, wo_sem, s0, r0, s1, r1, s2, r2, s3, r3, s4, r4, s5, r5, res_sem, fin_sem) = rest
    g = pl.program_id(0)
    t, n = lax.div(g, S), lax.rem(g, S)
    me = lax.axis_index("tp")
    core, yb, xb = lax.rem(me, 2), lax.rem(lax.div(me, 2), 2), lax.div(me, 4)
    to_core, to_y, to_x = me + 1 - 2 * core, me + 2 - 4 * yb, me + 4 - 8 * xb
    first, second = (xb, yb), (yb, xb)
    to_first, to_second = (to_x, to_y), (to_y, to_x)

    def remote(src, dst, send_sem, recv_sem, to):
        return pltpu.make_async_remote_copy(src_ref=src, dst_ref=dst, send_sem=send_sem, recv_sem=recv_sem, device_id={"tp": to},
                                            device_id_type=pl.DeviceIdType.MESH)

    def rows_of(u, piece, count):
        row = pl.multiple_of(lax.div(u, S) * R + piece * N, N)
        return pl.ds(row, count * N), pl.ds(pl.multiple_of(lax.rem(u, S) * BN, BN), BN)

    def own(h):
        return core * 8 + h * 4 + first[h] * 2 + second[h]

    def weights():
        return [pltpu.make_async_copy(w, wkv_s.at[:, pl.ds(i * HEAD, HEAD)], w_sem.at[i]) for i, w in enumerate((wk_hbm, wv_hbm))]

    def queries(i):
        at = pl.ds(pl.multiple_of(i * 2 * HEAD, 2 * HEAD), 2 * HEAD)
        return pltpu.make_async_copy(wq_hbm.at[:, at], wq_s.at[lax.rem(i, 2)], wq_sem.at[lax.rem(i, 2)])

    def columns(u):
        at = pl.ds(pl.multiple_of(lax.rem(u, S) * BN, BN), BN)
        return pltpu.make_async_copy(wo_hbm.at[:, at], wo_s.at[lax.rem(u, 2)], wo_sem.at[lax.rem(u, 2)])

    def sum0(u):
        a, b = lax.rem(u, 2), lax.rem(u, SLOTS)
        return remote(send0.at[a], recv0.at[b], s0.at[b], r0.at[b], to_core)

    def sum1(u, h):
        b = lax.rem(u, SLOTS)
        return remote(send1.at[b, h], recv1.at[b, h], s1.at[b, h], r1.at[b, h], to_first[h])

    def sum2(u, h):
        b = lax.rem(u, SLOTS)
        return remote(send2.at[b, h], recv2.at[b, h], s2.at[b, h], r2.at[b, h], to_second[h])

    def residual(u, h):
        b = lax.rem(u, SLOTS)
        return pltpu.make_async_copy(x_hbm.at[rows_of(u, own(h), 1)], res_s.at[b, h], res_sem.at[b, h])

    def stay(u, h):
        b = lax.rem(u, SLOTS)
        return pltpu.make_async_copy(fin_s.at[b, h], y_hbm.at[rows_of(u, own(h), 1)], fin_sem.at[b, h])

    def late(u, h, i):
        row = pl.multiple_of(second[h] * N, N)
        return lates[2 * i + h].at[pl.ds(row, N), pl.ds(pl.multiple_of(lax.rem(u, S) * BN, BN), BN)]

    def stay_late(u, h, i):
        b = lax.rem(u, SLOTS)
        return pltpu.make_async_copy(fin_s.at[b, h], late(u, h, i), fin_sem.at[b, h])

    def back3(u, h):
        b = lax.rem(u, SLOTS)
        return remote(fin_s.at[b, h], y_hbm.at[rows_of(u, own(h), 1)], s3.at[b, h], r3.at[b, h], to_second[h])

    def back3_late(u, h, i):
        b = lax.rem(u, SLOTS)
        return remote(fin_s.at[b, h], late(u, h, i), s3.at[b, h], r3.at[b, h], to_second[h])

    def back4(u, h):
        b = lax.rem(u, SLOTS)
        at = rows_of(u, core * 8 + h * 4 + first[h] * 2, 2)
        return remote(y_hbm.at[at], y_hbm.at[at], s4.at[b, h], r4.at[b, h], to_first[h])

    def back5(u):
        b = lax.rem(u, SLOTS)
        at = rows_of(u, core * 8, 8)
        return remote(y_hbm.at[at], y_hbm.at[at], s5.at[b], r5.at[b], to_core)

    @pl.when(g == 0)
    def _():
        barrier = pltpu.get_barrier_semaphore()
        for to in (to_core, to_y, to_x):
            pl.semaphore_signal(barrier, inc=1, device_id={"tp": to}, device_id_type=pl.DeviceIdType.MESH)
        for w in weights():
            w.start()
        queries(0).start()
        k_s[...] = jnp.zeros_like(k_s)
        vt_s[...] = jnp.zeros_like(vt_s)
        vt_s[HEAD:, :] = jnp.ones((16, ROWS), vt_s.dtype)

    @pl.when(g == S - 1)
    def _():
        pl.semaphore_wait(pltpu.get_barrier_semaphore(), 3)

    def at_step(stage):
        unit, on = 0, False
        for wait, first_unit, end in WAITS:
            u = g - S - 1 - wait * stage
            ok = (u >= first_unit) & (u < min(end, LATE if stage > F4 else UNITS))
            unit, on = jnp.where(ok, u, unit), on | ok
        return unit, on

    ahead = g + 1 - S

    @pl.when((ahead >= 0) & (ahead < UNITS))
    def _():
        columns(ahead).start()

    u6, on6 = at_step(F6)

    @pl.when(on6)
    def _():
        back5(u6).wait()

    u5, on5 = at_step(F5)

    @pl.when(on5)
    def _():
        for h in range(2):
            back4(u5, h).wait()
        back5(u5).start()

    u4, on4 = at_step(F4)

    @pl.when(on4)
    def _():
        for h in range(2):
            stay(u4, h).wait()
            back3(u4, h).wait()

        @pl.when(u4 < LATE)
        def _():
            for h in range(2):
                back4(u4, h).start()

    u3, on3 = at_step(J3)

    @pl.when(on3)
    def _():
        b = lax.rem(u3, SLOTS)
        for h in range(2):
            sum2(u3, h).wait()
            residual(u3, h).wait()
            total = keep2[b, h] + recv2[b, h].astype(jnp.float32) + res_s[b, h].astype(jnp.float32)
            fin_s[b, h] = total.astype(jnp.bfloat16)

        @pl.when(u3 < LATE)
        def _():
            for h in range(2):
                back3(u3, h).start()
                stay(u3, h).start()

        for i in range(TAIL):

            @pl.when(lax.div(u3, S) == C - TAIL + i)
            def _():
                for h in range(2):
                    back3_late(u3, h, i).start()
                    stay_late(u3, h, i).start()

    u2, on2 = at_step(J2)

    @pl.when(on2)
    def _():
        b = lax.rem(u2, SLOTS)
        for h in range(2):
            residual(u2, h).start()
            sum1(u2, h).wait()
            total = keep1[b, h] + recv1[b, h].astype(jnp.float32)
            send2[b, h] = total[:N].astype(jnp.bfloat16)
            keep2[b, h] = total[N:]
            sum2(u2, h).start()

    u1, on1 = at_step(J1)

    @pl.when(on1)
    def _():
        b = lax.rem(u1, SLOTS)
        sum0(u1).wait()
        for h in range(2):
            at = slice(h * 4 * N, (h + 1) * 4 * N)
            total = keep0[lax.rem(u1, 2), at] + recv0[b, at].astype(jnp.float32)
            send1[b, h] = total[: 2 * N].astype(jnp.bfloat16)
            keep1[b, h] = total[2 * N :]
            sum1(u1, h).start()

    u0 = g - S
    on0 = (u0 >= 0) & (u0 < UNITS)

    @pl.when(on0)
    def _():
        a = lax.rem(u0, 2)
        columns(u0).wait()
        term = jnp.dot(seen_s[lax.rem(lax.div(u0, S), 2)], wo_s[a], preferred_element_type=jnp.float32)
        send0[a] = term[: R // 2].astype(jnp.bfloat16)
        keep0[a] = term[R // 2 :]
        sum0(u0).start()

    pre = t < C

    @pl.when(pre & (n < NB))
    def _():
        groups, width = range(0, RB, 16), 1024
        scales = []
        for r in groups:
            squares = jnp.zeros((16, width), jnp.float32)
            for c in range(0, D, width):
                wide = x_ref[r : r + 16, c : c + width].astype(jnp.float32)
                squares += wide * wide
            scales.append(lax.rsqrt(jnp.sum(squares, -1, keepdims=True) * (1 / D) + 1e-6))
        for c in range(0, D, width):
            gain = gain_ref[c : c + width].astype(jnp.float32)[None, :]
            for r, scale in zip(groups, scales):
                at = pl.multiple_of(n * RB + r, 16)
                wide = x_ref[r : r + 16, c : c + width].astype(jnp.float32)
                normed_s[pl.ds(at, 16), c : c + width] = (wide * scale * gain).astype(jnp.bfloat16)

    place = pl.ds(pl.multiple_of(t * R, R), R)

    @pl.when(pre & (n == NB))
    def _():
        @pl.when(t == 0)
        def _():
            for w in weights():
                w.wait()

        kv = jnp.dot(normed_s[...], wkv_s[...], preferred_element_type=jnp.float32).astype(jnp.bfloat16).astype(jnp.float32)
        table, half = table_ref[place, :], HEAD // 2
        turn_s[0] = jnp.concatenate([table[:, :half], table[:, :half]], axis=1)
        turn_s[1] = jnp.concatenate([-table[:, half:], table[:, half:]], axis=1)
        k_s[place, :] = _turn(kv[:, :HEAD], turn_s[0], turn_s[1])
        vt_s[:HEAD, place] = kv[:, HEAD:].T.astype(jnp.bfloat16)

    pair = n - NB - 1

    @pl.when((n == S - 1) & (t + 1 < C))
    def _():
        queries(0).start()

    @pl.when(pre & (pair >= 0) & (pair < PAIRS))
    def _():
        @pl.when(pair + 1 < PAIRS)
        def _():
            queries(pair + 1).start()

        queries(pair).wait()
        q = jnp.dot(normed_s[...], wq_s[lax.rem(pair, 2)], preferred_element_type=jnp.float32).astype(jnp.bfloat16).astype(jnp.float32)
        for i in range(2):
            q_s[lax.rem(pair, 2), i * R : (i + 1) * R, :] = _turn(q[:, i * HEAD : (i + 1) * HEAD], turn_s[0], turn_s[1])

    @pl.when(pre & (pair >= 1))
    def _():
        q_ref = q_s.at[lax.rem(pair - 1, 2)]
        cols = 2 * R
        top_s[...] = jnp.full(top_s.shape, NEG, jnp.float32)
        mix_s[...] = jnp.zeros(mix_s.shape, jnp.float32)

        def block(first_key, bk, masked):
            here = pl.ds(pl.multiple_of(first_key, bk), bk)
            s = _dot(k_s[here, :], q_ref[...], 1, 1)
            if masked:
                key = first_key + lax.broadcasted_iota(jnp.int32, (bk, cols), 0)
                query = t * R + lax.rem(lax.broadcasted_iota(jnp.int32, (bk, cols), 1), R)
                s = jnp.where(key <= query, s, HIDDEN)
            old = top_s[0:1, :]
            top = jnp.maximum(old, s.max(axis=0, keepdims=True))
            top_s[0:1, :] = top
            p = jnp.exp2((s - top) * E).astype(jnp.bfloat16)
            mix_s[...] = mix_s[...] * jnp.exp2((old - top) * E) + _dot(vt_s[:, here], p, 1, 0)

        whole = lax.div(t * R, BK)
        lax.fori_loop(0, whole, lambda j, _: block(j * BK, BK, False), None)

        @pl.when(whole * BK < t * R)
        def _():
            block(whole * BK, BK, True)

        @pl.when(whole * BK == t * R)
        def _():
            block(t * R, R, True)

        out = (mix_s[:HEAD, :] * (1 / mix_s[HEAD : HEAD + 1, :])).T.astype(jnp.bfloat16)
        head = (pair - 1) * 2
        for p in range(16):
            c, h, b1, b2 = p >> 3, (p >> 2) & 1, (p >> 1) & 1, p & 1
            kept = lambda bit, mine: mine if bit else 1 - mine
            to = (kept(c, core) * 2 + h) * 4 + kept(b1, first[h]) * 2 + kept(b2, second[h])
            for i in range(2):
                at = pl.ds(pl.multiple_of((head + i) * HEAD, HEAD), HEAD)
                seen_s[lax.rem(t, 2), pl.ds(pl.multiple_of(to * N, N), N), at] = out[i * R + p * N : i * R + (p + 1) * N, :]


def _attention(x, gain, wq, wk, wv, wo):
    width = wq.shape[1]
    hbm = pl.BlockSpec(memory_space=pl.ANY)
    once = pl.Buffered(1)
    div, rem = lax.div, lax.rem

    def x_block(g):
        ahead = jnp.where(rem(g, S) >= NB, div(g, S) * NB + NB, div(g, S) * NB + rem(g, S))
        return jnp.minimum(ahead, ROWS // RB - 1), 0

    bf, f32 = jnp.bfloat16, jnp.float32
    dma = pltpu.SemaphoreType.DMA
    return pl.pallas_call(
        _kernel,
        grid=(STEPS,),
        in_specs=[
            pl.BlockSpec((RB, D), x_block),
            pl.BlockSpec((D,), lambda g: (0,), pipeline_mode=once),
            pl.BlockSpec((ROWS, HEAD), lambda g: (0, 0), pipeline_mode=once),
            hbm, hbm, hbm, hbm, hbm,
        ],
        out_specs=[hbm] * (1 + 2 * TAIL),
        out_shape=[jax.ShapeDtypeStruct((n, D), bf) for n in (ROWS, *[2 * N] * (2 * TAIL))],
        scratch_shapes=[
            pltpu.VMEM((R, D), bf),
            pltpu.VMEM((D, 2 * HEAD), bf),
            pltpu.VMEM((2, D, 2 * HEAD), bf),
            pltpu.VMEM((2, width, BN), bf),
            pltpu.VMEM((ROWS, HEAD), bf),
            pltpu.VMEM((HEAD + 16, ROWS), bf),
            pltpu.VMEM((2, R, width), bf),
            pltpu.VMEM((2, R, HEAD), f32),
            pltpu.VMEM((2, 2 * R, HEAD), bf),
            pltpu.VMEM((8, 2 * R), f32),
            pltpu.VMEM((HEAD + 16, 2 * R), f32),
            pltpu.VMEM((2, R // 2, BN), bf), pltpu.VMEM((2, R // 2, BN), f32), pltpu.VMEM((SLOTS, R // 2, BN), bf),
            pltpu.VMEM((SLOTS, 2, 2 * N, BN), bf), pltpu.VMEM((SLOTS, 2, 2 * N, BN), f32), pltpu.VMEM((SLOTS, 2, 2 * N, BN), bf),
            pltpu.VMEM((SLOTS, 2, N, BN), bf), pltpu.VMEM((SLOTS, 2, N, BN), f32), pltpu.VMEM((SLOTS, 2, N, BN), bf),
            pltpu.VMEM((SLOTS, 2, N, BN), bf), pltpu.VMEM((SLOTS, 2, N, BN), bf),
            dma((2,)), dma((2,)), dma((2,)),
            dma((SLOTS,)), dma((SLOTS,)), dma((SLOTS, 2)), dma((SLOTS, 2)), dma((SLOTS, 2)), dma((SLOTS, 2)),
            dma((SLOTS, 2)), dma((SLOTS, 2)), dma((SLOTS, 2)), dma((SLOTS, 2)), dma((SLOTS,)), dma((SLOTS,)),
            dma((SLOTS, 2)), dma((SLOTS, 2)),
        ],
        compiler_params=pltpu.CompilerParams(dimension_semantics=("arbitrary",), vmem_limit_bytes=64 * 2**20 - 65536, collective_id=0,
                                             has_side_effects=True),
        cost_estimate=pl.CostEstimate(flops=2 * ROWS * D * (2 * width + 2 * HEAD), transcendentals=0, bytes_accessed=C * 4 * D * width),
        name="layer",
    )(x, gain, _table(), x, wq, wk, wv, wo)


def _move_kernel(blocks, src_ref, *rest):
    dst_ref, buf, in_sem, out_sem = rest[-4:]
    ring, rb = buf.shape[0], buf.shape[1]
    at = lambda i: pl.ds(blocks[i] * rb, rb)
    get = lambda i: pltpu.make_async_copy(src_ref.at[at(i)], buf.at[i % ring], in_sem.at[i % ring])
    put = lambda i: pltpu.make_async_copy(buf.at[i % ring], dst_ref.at[at(i)], out_sem.at[i % ring])
    count, lag = len(blocks), ring // 2
    for i in range(count + lag):
        if i < count:
            if i >= ring:
                put(i - ring).wait()
            get(i).start()
        if i >= lag:
            get(i - lag).wait()
            put(i - lag).start()
    for i in range(max(count - ring, 0), count):
        put(i).wait()


def _move(src, dst, row0, row1):
    rb, ring = 64, 12
    hbm = pl.BlockSpec(memory_space=pl.ANY)
    args = (src,) if dst is None else (src, dst)
    return pl.pallas_call(
        functools.partial(_move_kernel, tuple(range(row0 // rb, row1 // rb))),
        in_specs=[hbm] * len(args),
        out_specs=hbm,
        out_shape=jax.ShapeDtypeStruct((ROWS, D), jnp.bfloat16),
        scratch_shapes=[pltpu.VMEM((ring, rb, D), jnp.bfloat16), pltpu.SemaphoreType.DMA((ring,)), pltpu.SemaphoreType.DMA((ring,))],
        input_output_aliases={} if dst is None else {1: 0},
        compiler_params=pltpu.CompilerParams(vmem_limit_bytes=48 * 2**20),
        cost_estimate=pl.CostEstimate(flops=(row1 - row0) * D * 2000, transcendentals=0, bytes_accessed=(row1 - row0) * D * 4),
        name="move",
    )(*args)


def _place_kernel(where, *refs):
    pieces, (y_ref, buf, in_sem, out_sem) = refs[: len(where)], refs[-4:]
    me = lax.axis_index("tp")
    core, yb, xb = lax.rem(me, 2), lax.rem(lax.div(me, 2), 2), lax.div(me, 4)
    gets, puts = [], []
    for i, (piece, (row0, other, h, moved)) in enumerate(zip(pieces, where)):
        n = piece.shape[0]
        c = 1 - core if other else core
        p1 = (xb, yb)[h]
        p1 = 1 - p1 if moved else p1
        at = pl.multiple_of(row0 + (c * 4 + h * 2 + p1) * n, n)
        gets.append(pltpu.make_async_copy(piece, buf.at[i], in_sem.at[i]))
        puts.append(pltpu.make_async_copy(buf.at[i], y_ref.at[pl.ds(at, n)], out_sem.at[i]))
    for get in gets:
        get.start()
    for get, put in zip(gets, puts):
        get.wait()
        put.start()
    for put in puts:
        put.wait()


def _place(items, y):
    where, pieces = zip(*items)
    count, n = len(pieces), pieces[0].shape[0]
    hbm = pl.BlockSpec(memory_space=pl.ANY)
    return pl.pallas_call(
        functools.partial(_place_kernel, where),
        in_specs=[hbm] * (count + 1),
        out_specs=hbm,
        out_shape=jax.ShapeDtypeStruct((ROWS, D), jnp.bfloat16),
        scratch_shapes=[pltpu.VMEM((count, n, D), jnp.bfloat16), pltpu.SemaphoreType.DMA((count,)), pltpu.SemaphoreType.DMA((count,))],
        input_output_aliases={count: 0},
        compiler_params=pltpu.CompilerParams(vmem_limit_bytes=32 * 2**20),
        cost_estimate=pl.CostEstimate(flops=count * n * D * 2000, transcendentals=0, bytes_accessed=count * n * D * 4),
        name="place",
    )(*pieces, y)


def solution(mesh):
    def swap(t, bit):
        return lax.ppermute(t, "tp", [(i, i ^ bit) for i in range(8)])

    def step(x, gain, wq, wk, wv, wo):
        y, *lates = _attention(x, gain, wq, wk, wv, wo)
        owns = [lates[2 * i : 2 * i + 2] for i in range(TAIL)]
        alongs = [[swap(a, 4), swap(b, 2)] for a, b in owns]
        others = [[swap(a, 1), swap(b, 1)] for a, b in owns]
        rows = [ROWS - (TAIL - i) * R for i in range(TAIL)]
        ends = [0, 14 * RB, ROWS - TAIL * R]
        done, ready = None, []
        for i in range(TAIL):
            done = _move(y, done, ends[i], ends[i + 1])
            for h in range(2):
                ready += [((rows[i], 0, h, 0), owns[i][h]), ((rows[i], 1, h, 0), others[i][h])]
            if i < TAIL - 1:
                alongs[i], done = lax.optimization_barrier((alongs[i], done))
                for h in range(2):
                    ready += [((rows[i], 0, h, 1), alongs[i][h]), ((rows[i], 1, h, 1), swap(alongs[i][h], 1))]
        done = _place(ready, done)
        last, done = lax.optimization_barrier((alongs[-1], done))
        far = [swap(t, 1) for t in last]
        done = _place([((rows[-1], 0, h, 1), last[h]) for h in range(2)], done)
        far, done = lax.optimization_barrier((far, done))
        return _place([((rows[-1], 1, h, 1), far[h]) for h in range(2)], done)

    tokens, columns = P("dp", None), P(None, "tp")
    return jax.shard_map(
        step,
        mesh=mesh,
        in_specs=(tokens, P(None), columns, columns, columns, P("tp", None)),
        out_specs=tokens,
        check_vma=False,
    )
```

```python
import functools

import jax
import jax.numpy as jnp
import numpy as np
from jax import lax
from jax.experimental import pallas as pl
from jax.experimental.pallas import tpu as pltpu
from jax.sharding import PartitionSpec as P

HEAD = 128
THETA = 10000
NEG = -1e30
HIDDEN = 2 * NEG
LOG2E = 1.4426950408889634
E = HEAD**-0.5 * LOG2E
ROWS, D = 2048, 12288
R = 256
S = 12
BN = D // S
RB = 64
BK = 512
C = ROWS // R
UNITS = C * S
N = R // 16
SLOTS = 8
J1, J2, J3, F4, F5, F6 = range(6)
WAITS = ((2, 0, 8), (3, 8, 20), (4, 20, UNITS))
TAIL = 2
LATE = UNITS - TAIL * S
STEPS = S + UNITS + 1 + WAITS[-1][0] * F4
NB = R // RB
PAIRS = S - NB - 2


def _dot(a, b, ca, cb):
    return lax.dot_general(a, b, (((ca,), (cb,)), ((), ())), preferred_element_type=jnp.float32)


def _table():
    half = HEAD // 2
    freq = (np.float32(THETA) ** (-np.arange(half, dtype=np.float32) / np.float32(half))).astype(np.float32)
    angle = np.arange(ROWS, dtype=np.float32)[:, None] * freq
    return np.concatenate([np.cos(angle), np.sin(angle)], axis=1).astype(np.float32)


def _turn(t, cos, sin):
    return (t * cos + pltpu.roll(t, HEAD // 2, 1) * sin).astype(jnp.bfloat16)


def _kernel(x_ref, gain_ref, table_ref, x_hbm, wq_hbm, wk_hbm, wv_hbm, wo_hbm, y_hbm, *rest):
    lates, rest = rest[: 2 * TAIL], rest[2 * TAIL :]
    (normed_s, wkv_s, wq_s, wo_s, k_s, vt_s, seen_s, turn_s, q_s, top_s, mix_s,
     send0, keep0, recv0, send1, keep1, recv1, send2, keep2, recv2, res_s, fin_s,
     w_sem, wq_sem, wo_sem, s0, r0, s1, r1, s2, r2, s3, r3, s4, r4, s5, r5, res_sem, fin_sem) = rest
    g = pl.program_id(0)
    t, n = lax.div(g, S), lax.rem(g, S)
    me = lax.axis_index("tp")
    core, yb, xb = lax.rem(me, 2), lax.rem(lax.div(me, 2), 2), lax.div(me, 4)
    to_core, to_y, to_x = me + 1 - 2 * core, me + 2 - 4 * yb, me + 4 - 8 * xb
    first, second = (xb, yb), (yb, xb)
    to_first, to_second = (to_x, to_y), (to_y, to_x)

    def remote(src, dst, send_sem, recv_sem, to):
        return pltpu.make_async_remote_copy(src_ref=src, dst_ref=dst, send_sem=send_sem, recv_sem=recv_sem, device_id={"tp": to},
                                            device_id_type=pl.DeviceIdType.MESH)

    def rows_of(u, piece, count):
        row = pl.multiple_of(lax.div(u, S) * R + piece * N, N)
        return pl.ds(row, count * N), pl.ds(pl.multiple_of(lax.rem(u, S) * BN, BN), BN)

    def own(h):
        return core * 8 + h * 4 + first[h] * 2 + second[h]

    def weights():
        return [pltpu.make_async_copy(w, wkv_s.at[:, pl.ds(i * HEAD, HEAD)], w_sem.at[i]) for i, w in enumerate((wk_hbm, wv_hbm))]

    def queries(i):
        at = pl.ds(pl.multiple_of(i * 2 * HEAD, 2 * HEAD), 2 * HEAD)
        return pltpu.make_async_copy(wq_hbm.at[:, at], wq_s.at[lax.rem(i, 2)], wq_sem.at[lax.rem(i, 2)])

    def columns(u):
        at = pl.ds(pl.multiple_of(lax.rem(u, S) * BN, BN), BN)
        return pltpu.make_async_copy(wo_hbm.at[:, at], wo_s.at[lax.rem(u, 2)], wo_sem.at[lax.rem(u, 2)])

    def sum0(u):
        a, b = lax.rem(u, 2), lax.rem(u, SLOTS)
        return remote(send0.at[a], recv0.at[b], s0.at[b], r0.at[b], to_core)

    def sum1(u, h):
        b = lax.rem(u, SLOTS)
        return remote(send1.at[b, h], recv1.at[b, h], s1.at[b, h], r1.at[b, h], to_first[h])

    def sum2(u, h):
        b = lax.rem(u, SLOTS)
        return remote(send2.at[b, h], recv2.at[b, h], s2.at[b, h], r2.at[b, h], to_second[h])

    def residual(u, h):
        b = lax.rem(u, SLOTS)
        return pltpu.make_async_copy(x_hbm.at[rows_of(u, own(h), 1)], res_s.at[b, h], res_sem.at[b, h])

    def stay(u, h):
        b = lax.rem(u, SLOTS)
        return pltpu.make_async_copy(fin_s.at[b, h], y_hbm.at[rows_of(u, own(h), 1)], fin_sem.at[b, h])

    def late(u, h, i):
        row = pl.multiple_of(second[h] * N, N)
        return lates[2 * i + h].at[pl.ds(row, N), pl.ds(pl.multiple_of(lax.rem(u, S) * BN, BN), BN)]

    def stay_late(u, h, i):
        b = lax.rem(u, SLOTS)
        return pltpu.make_async_copy(fin_s.at[b, h], late(u, h, i), fin_sem.at[b, h])

    def back3(u, h):
        b = lax.rem(u, SLOTS)
        return remote(fin_s.at[b, h], y_hbm.at[rows_of(u, own(h), 1)], s3.at[b, h], r3.at[b, h], to_second[h])

    def back3_late(u, h, i):
        b = lax.rem(u, SLOTS)
        return remote(fin_s.at[b, h], late(u, h, i), s3.at[b, h], r3.at[b, h], to_second[h])

    def back4(u, h):
        b = lax.rem(u, SLOTS)
        at = rows_of(u, core * 8 + h * 4 + first[h] * 2, 2)
        return remote(y_hbm.at[at], y_hbm.at[at], s4.at[b, h], r4.at[b, h], to_first[h])

    def back5(u):
        b = lax.rem(u, SLOTS)
        at = rows_of(u, core * 8, 8)
        return remote(y_hbm.at[at], y_hbm.at[at], s5.at[b], r5.at[b], to_core)

    @pl.when(g == 0)
    def _():
        barrier = pltpu.get_barrier_semaphore()
        for to in (to_core, to_y, to_x):
            pl.semaphore_signal(barrier, inc=1, device_id={"tp": to}, device_id_type=pl.DeviceIdType.MESH)
        for w in weights():
            w.start()
        vt_s[HEAD:, :] = jnp.ones((16, ROWS), vt_s.dtype)

    @pl.when(g == 3)
    def _():
        queries(0).start()

    @pl.when(g == S - 1)
    def _():
        pl.semaphore_wait(pltpu.get_barrier_semaphore(), 3)

    def at_step(stage):
        unit, on = 0, False
        for wait, first_unit, end in WAITS:
            u = g - S - 1 - wait * stage
            ok = (u >= first_unit) & (u < min(end, LATE if stage > F4 else UNITS))
            unit, on = jnp.where(ok, u, unit), on | ok
        return unit, on

    ahead = g + 1 - S

    @pl.when((ahead >= 0) & (ahead < UNITS))
    def _():
        columns(ahead).start()

    u6, on6 = at_step(F6)

    @pl.when(on6)
    def _():
        back5(u6).wait()

    u5, on5 = at_step(F5)

    @pl.when(on5)
    def _():
        for h in range(2):
            back4(u5, h).wait()
        back5(u5).start()

    u4, on4 = at_step(F4)

    @pl.when(on4)
    def _():
        for h in range(2):
            stay(u4, h).wait()
            back3(u4, h).wait()

        @pl.when(u4 < LATE)
        def _():
            for h in range(2):
                back4(u4, h).start()

    u3, on3 = at_step(J3)

    @pl.when(on3)
    def _():
        b = lax.rem(u3, SLOTS)
        for h in range(2):
            sum2(u3, h).wait()
            residual(u3, h).wait()
            total = keep2[b, h] + recv2[b, h].astype(jnp.float32) + res_s[b, h].astype(jnp.float32)
            fin_s[b, h] = total.astype(jnp.bfloat16)

        @pl.when(u3 < LATE)
        def _():
            for h in range(2):
                back3(u3, h).start()
                stay(u3, h).start()

        for i in range(TAIL):

            @pl.when(lax.div(u3, S) == C - TAIL + i)
            def _():
                for h in range(2):
                    back3_late(u3, h, i).start()
                    stay_late(u3, h, i).start()

    u2, on2 = at_step(J2)

    @pl.when(on2)
    def _():
        b = lax.rem(u2, SLOTS)
        for h in range(2):
            residual(u2, h).start()
            sum1(u2, h).wait()
            total = keep1[b, h] + recv1[b, h].astype(jnp.float32)
            send2[b, h] = total[:N].astype(jnp.bfloat16)
            keep2[b, h] = total[N:]
            sum2(u2, h).start()

    u1, on1 = at_step(J1)

    @pl.when(on1)
    def _():
        b = lax.rem(u1, SLOTS)
        sum0(u1).wait()
        for h in range(2):
            at = slice(h * 4 * N, (h + 1) * 4 * N)
            total = keep0[lax.rem(u1, 2), at] + recv0[b, at].astype(jnp.float32)
            send1[b, h] = total[: 2 * N].astype(jnp.bfloat16)
            keep1[b, h] = total[2 * N :]
            sum1(u1, h).start()

    u0 = g - S
    on0 = (u0 >= 0) & (u0 < UNITS)

    @pl.when(on0)
    def _():
        a = lax.rem(u0, 2)
        columns(u0).wait()
        term = jnp.dot(seen_s[lax.rem(lax.div(u0, S), 2)], wo_s[a], preferred_element_type=jnp.float32)
        send0[a] = term[: R // 2].astype(jnp.bfloat16)
        keep0[a] = term[R // 2 :]
        sum0(u0).start()

    pre = t < C

    @pl.when(pre & (n < NB))
    def _():
        groups, width = range(0, RB, 16), 1024
        scales = []
        for r in groups:
            squares = jnp.zeros((16, width), jnp.float32)
            for c in range(0, D, width):
                wide = x_ref[r : r + 16, c : c + width].astype(jnp.float32)
                squares += wide * wide
            scales.append(lax.rsqrt(jnp.sum(squares, -1, keepdims=True) * (1 / D) + 1e-6))
        for c in range(0, D, width):
            gain = gain_ref[c : c + width].astype(jnp.float32)[None, :]
            for r, scale in zip(groups, scales):
                at = pl.multiple_of(n * RB + r, 16)
                wide = x_ref[r : r + 16, c : c + width].astype(jnp.float32)
                normed_s[pl.ds(at, 16), c : c + width] = (wide * scale * gain).astype(jnp.bfloat16)

    place = pl.ds(pl.multiple_of(t * R, R), R)

    @pl.when(pre & (n == NB))
    def _():
        @pl.when(t == 0)
        def _():
            for w in weights():
                w.wait()

        kv = jnp.dot(normed_s[...], wkv_s[...], preferred_element_type=jnp.float32).astype(jnp.bfloat16).astype(jnp.float32)
        table, half = table_ref[...], HEAD // 2
        turn_s[0] = jnp.concatenate([table[:, :half], table[:, :half]], axis=1)
        turn_s[1] = jnp.concatenate([-table[:, half:], table[:, half:]], axis=1)
        k_s[place, :] = _turn(kv[:, :HEAD], turn_s[0], turn_s[1])
        vt_s[:HEAD, place] = kv[:, HEAD:].T.astype(jnp.bfloat16)

    pair = n - NB - 1

    @pl.when((n == S - 1) & (t + 1 < C))
    def _():
        queries(0).start()

    @pl.when(pre & (pair >= 0) & (pair < PAIRS))
    def _():
        @pl.when(pair + 1 < PAIRS)
        def _():
            queries(pair + 1).start()

        queries(pair).wait()
        q = jnp.dot(normed_s[...], wq_s[lax.rem(pair, 2)], preferred_element_type=jnp.float32).astype(jnp.bfloat16).astype(jnp.float32)
        for i in range(2):
            q_s[lax.rem(pair, 2), i * R : (i + 1) * R, :] = _turn(q[:, i * HEAD : (i + 1) * HEAD], turn_s[0], turn_s[1])

    @pl.when(pre & (pair >= 1))
    def _():
        q_ref = q_s.at[lax.rem(pair - 1, 2)]
        cols = 2 * R
        top_s[...] = jnp.full(top_s.shape, NEG, jnp.float32)
        mix_s[...] = jnp.zeros(mix_s.shape, jnp.float32)

        def block(first_key, bk, masked):
            here = pl.ds(pl.multiple_of(first_key, bk), bk)
            s = _dot(k_s[here, :], q_ref[...], 1, 1)
            if masked:
                key = first_key + lax.broadcasted_iota(jnp.int32, (bk, cols), 0)
                query = t * R + lax.rem(lax.broadcasted_iota(jnp.int32, (bk, cols), 1), R)
                s = jnp.where(key <= query, s, HIDDEN)
            old = top_s[0:1, :]
            top = jnp.maximum(old, s.max(axis=0, keepdims=True))
            top_s[0:1, :] = top
            p = jnp.exp2((s - top) * E).astype(jnp.bfloat16)
            mix_s[...] = mix_s[...] * jnp.exp2((old - top) * E) + _dot(vt_s[:, here], p, 1, 0)

        whole = lax.div(t * R, BK)
        lax.fori_loop(0, whole, lambda j, _: block(j * BK, BK, False), None)

        @pl.when(whole * BK < t * R)
        def _():
            block(whole * BK, BK, True)

        @pl.when(whole * BK == t * R)
        def _():
            block(t * R, R, True)

        out = (mix_s[:HEAD, :] * (1 / mix_s[HEAD : HEAD + 1, :])).T.astype(jnp.bfloat16)
        head = (pair - 1) * 2
        for p in range(16):
            c, h, b1, b2 = p >> 3, (p >> 2) & 1, (p >> 1) & 1, p & 1
            kept = lambda bit, mine: mine if bit else 1 - mine
            to = (kept(c, core) * 2 + h) * 4 + kept(b1, first[h]) * 2 + kept(b2, second[h])
            for i in range(2):
                at = pl.ds(pl.multiple_of((head + i) * HEAD, HEAD), HEAD)
                seen_s[lax.rem(t, 2), pl.ds(pl.multiple_of(to * N, N), N), at] = out[i * R + p * N : i * R + (p + 1) * N, :]


def _attention(x, gain, wq, wk, wv, wo):
    width = wq.shape[1]
    hbm = pl.BlockSpec(memory_space=pl.ANY)
    once = pl.Buffered(1)
    div, rem = lax.div, lax.rem

    def x_block(g):
        ahead = jnp.where(rem(g, S) >= NB, div(g, S) * NB + NB, div(g, S) * NB + rem(g, S))
        return jnp.minimum(ahead, ROWS // RB - 1), 0

    bf, f32 = jnp.bfloat16, jnp.float32
    dma = pltpu.SemaphoreType.DMA
    return pl.pallas_call(
        _kernel,
        grid=(STEPS,),
        in_specs=[
            pl.BlockSpec((RB, D), x_block),
            pl.BlockSpec((D,), lambda g: (0,), pipeline_mode=once),
            pl.BlockSpec((R, HEAD), lambda g: (jnp.minimum(div(g, S), C - 1), 0)),
            hbm, hbm, hbm, hbm, hbm,
        ],
        out_specs=[hbm] * (1 + 2 * TAIL),
        out_shape=[jax.ShapeDtypeStruct((n, D), bf) for n in (ROWS, *[2 * N] * (2 * TAIL))],
        scratch_shapes=[
            pltpu.VMEM((R, D), bf),
            pltpu.VMEM((D, 2 * HEAD), bf),
            pltpu.VMEM((2, D, 2 * HEAD), bf),
            pltpu.VMEM((2, width, BN), bf),
            pltpu.VMEM((ROWS, HEAD), bf),
            pltpu.VMEM((HEAD + 16, ROWS), bf),
            pltpu.VMEM((2, R, width), bf),
            pltpu.VMEM((2, R, HEAD), f32),
            pltpu.VMEM((2, 2 * R, HEAD), bf),
            pltpu.VMEM((8, 2 * R), f32),
            pltpu.VMEM((HEAD + 16, 2 * R), f32),
            pltpu.VMEM((2, R // 2, BN), bf), pltpu.VMEM((2, R // 2, BN), f32), pltpu.VMEM((SLOTS, R // 2, BN), bf),
            pltpu.VMEM((SLOTS, 2, 2 * N, BN), bf), pltpu.VMEM((SLOTS, 2, 2 * N, BN), f32), pltpu.VMEM((SLOTS, 2, 2 * N, BN), bf),
            pltpu.VMEM((SLOTS, 2, N, BN), bf), pltpu.VMEM((SLOTS, 2, N, BN), f32), pltpu.VMEM((SLOTS, 2, N, BN), bf),
            pltpu.VMEM((SLOTS, 2, N, BN), bf), pltpu.VMEM((SLOTS, 2, N, BN), bf),
            dma((2,)), dma((2,)), dma((2,)),
            dma((SLOTS,)), dma((SLOTS,)), dma((SLOTS, 2)), dma((SLOTS, 2)), dma((SLOTS, 2)), dma((SLOTS, 2)),
            dma((SLOTS, 2)), dma((SLOTS, 2)), dma((SLOTS, 2)), dma((SLOTS, 2)), dma((SLOTS,)), dma((SLOTS,)),
            dma((SLOTS, 2)), dma((SLOTS, 2)),
        ],
        compiler_params=pltpu.CompilerParams(dimension_semantics=("arbitrary",), vmem_limit_bytes=64 * 2**20 - 65536, collective_id=0,
                                             has_side_effects=True),
        cost_estimate=pl.CostEstimate(flops=2 * ROWS * D * (2 * width + 2 * HEAD), transcendentals=0, bytes_accessed=C * 4 * D * width),
        name="layer",
    )(x, gain, _table(), x, wq, wk, wv, wo)


def _move_kernel(blocks, src_ref, *rest):
    dst_ref, buf, in_sem, out_sem = rest[-4:]
    ring, rb = buf.shape[0], buf.shape[1]
    at = lambda i: pl.ds(blocks[i] * rb, rb)
    get = lambda i: pltpu.make_async_copy(src_ref.at[at(i)], buf.at[i % ring], in_sem.at[i % ring])
    put = lambda i: pltpu.make_async_copy(buf.at[i % ring], dst_ref.at[at(i)], out_sem.at[i % ring])
    count, lag = len(blocks), ring // 2
    for i in range(count + lag):
        if i < count:
            if i >= ring:
                put(i - ring).wait()
            get(i).start()
        if i >= lag:
            get(i - lag).wait()
            put(i - lag).start()
    for i in range(max(count - ring, 0), count):
        put(i).wait()


def _move(src, dst, row0, row1):
    rb, ring = 64, 12
    hbm = pl.BlockSpec(memory_space=pl.ANY)
    args = (src,) if dst is None else (src, dst)
    return pl.pallas_call(
        functools.partial(_move_kernel, tuple(range(row0 // rb, row1 // rb))),
        in_specs=[hbm] * len(args),
        out_specs=hbm,
        out_shape=jax.ShapeDtypeStruct((ROWS, D), jnp.bfloat16),
        scratch_shapes=[pltpu.VMEM((ring, rb, D), jnp.bfloat16), pltpu.SemaphoreType.DMA((ring,)), pltpu.SemaphoreType.DMA((ring,))],
        input_output_aliases={} if dst is None else {1: 0},
        compiler_params=pltpu.CompilerParams(vmem_limit_bytes=48 * 2**20),
        cost_estimate=pl.CostEstimate(flops=(row1 - row0) * D * 2000, transcendentals=0, bytes_accessed=(row1 - row0) * D * 4),
        name="move",
    )(*args)


def _place_kernel(where, *refs):
    pieces, (y_ref, buf, in_sem, out_sem) = refs[: len(where)], refs[-4:]
    me = lax.axis_index("tp")
    core, yb, xb = lax.rem(me, 2), lax.rem(lax.div(me, 2), 2), lax.div(me, 4)
    gets, puts = [], []
    for i, (piece, (row0, other, h, moved)) in enumerate(zip(pieces, where)):
        n = piece.shape[0]
        c = 1 - core if other else core
        p1 = (xb, yb)[h]
        p1 = 1 - p1 if moved else p1
        at = pl.multiple_of(row0 + (c * 4 + h * 2 + p1) * n, n)
        gets.append(pltpu.make_async_copy(piece, buf.at[i], in_sem.at[i]))
        puts.append(pltpu.make_async_copy(buf.at[i], y_ref.at[pl.ds(at, n)], out_sem.at[i]))
    for get in gets:
        get.start()
    for get, put in zip(gets, puts):
        get.wait()
        put.start()
    for put in puts:
        put.wait()


def _place(items, y):
    where, pieces = zip(*items)
    count, n = len(pieces), pieces[0].shape[0]
    hbm = pl.BlockSpec(memory_space=pl.ANY)
    return pl.pallas_call(
        functools.partial(_place_kernel, where),
        in_specs=[hbm] * (count + 1),
        out_specs=hbm,
        out_shape=jax.ShapeDtypeStruct((ROWS, D), jnp.bfloat16),
        scratch_shapes=[pltpu.VMEM((count, n, D), jnp.bfloat16), pltpu.SemaphoreType.DMA((count,)), pltpu.SemaphoreType.DMA((count,))],
        input_output_aliases={count: 0},
        compiler_params=pltpu.CompilerParams(vmem_limit_bytes=32 * 2**20),
        cost_estimate=pl.CostEstimate(flops=count * n * D * 2000, transcendentals=0, bytes_accessed=count * n * D * 4),
        name="place",
    )(*pieces, y)


def solution(mesh):
    def swap(t, bit):
        return lax.ppermute(t, "tp", [(i, i ^ bit) for i in range(8)])

    def step(x, gain, wq, wk, wv, wo):
        y, *lates = _attention(x, gain, wq, wk, wv, wo)
        owns = [lates[2 * i : 2 * i + 2] for i in range(TAIL)]
        alongs = [[swap(a, 4), swap(b, 2)] for a, b in owns]
        others = [[swap(a, 1), swap(b, 1)] for a, b in owns]
        rows = [ROWS - (TAIL - i) * R for i in range(TAIL)]
        ends = [0, 14 * RB, ROWS - TAIL * R]
        done, ready = None, []
        for i in range(TAIL):
            done = _move(y, done, ends[i], ends[i + 1])
            for h in range(2):
                ready += [((rows[i], 0, h, 0), owns[i][h]), ((rows[i], 1, h, 0), others[i][h])]
            if i < TAIL - 1:
                alongs[i], done = lax.optimization_barrier((alongs[i], done))
                for h in range(2):
                    ready += [((rows[i], 0, h, 1), alongs[i][h]), ((rows[i], 1, h, 1), swap(alongs[i][h], 1))]
        done = _place(ready, done)
        last, done = lax.optimization_barrier((alongs[-1], done))
        far = [swap(t, 1) for t in last]
        done = _place([((rows[-1], 0, h, 1), last[h]) for h in range(2)], done)
        far, done = lax.optimization_barrier((far, done))
        return _place([((rows[-1], 1, h, 1), far[h]) for h in range(2)], done)

    tokens, columns = P("dp", None), P(None, "tp")
    return jax.shard_map(
        step,
        mesh=mesh,
        in_specs=(tokens, P(None), columns, columns, columns, P("tp", None)),
        out_specs=tokens,
        check_vma=False,
    )
```
